256 devices in a mesh: lat: 64 (over z_hi, y, x, core), ens: 4 (over z_lo).
Axes of the slice: x: 4, y: 4, z: 8 (z_hi: 2, z_lo: 4; z = z_hi * 4 + z_lo), core: 2. Of those that a mesh axis runs over, the one named last changes fastest.
Arguments:
- predicted_grid: bfloat16 [8, 36, 512, 1440], P('ens', None, 'lat'), may hold values from -6 to 6
- verifying_coefficients: float32 [36, 2, 128, 721], P(None, None, 'lat'), may hold values from -5 to 5
- weighted_polynomial_values: bfloat16 [128, 512, 721], P('lat'), may hold values from -0.25 to 0.25
- zonal_order_values: int32 [128], replicated, may hold values from 0 to 720, as said below
Outputs:
- prediction_sensitivity: bfloat16 [8, 36, 512, 1440], P('ens', None, 'lat')
- coefficient_error_mean: float32 [36, 2, 128], P(None, None, 'lat')
The draws below stay inside these ranges and needn't reach their ends.
Inputs may be any that keep to these rules, and one draw needn't show every extreme that they name: `zonal_order_values`: the wavenumbers are distinct, 0 and 720 are always among them; slot s belongs to index s // 2 of lat.
All inputs are finite; a program needn't handle non-finite values.
Results may differ from the reference program's by a relative error of at most 0.014.
Values may be sent and summed in bfloat16 or wider, within the bound.
No kernel may reach another device: no remote copies, remote signals or barrier semaphores. Data moves between devices by JAX's collectives and lax.ppermute only.
A program may use at most 64 MiB of HBM per device.

```python
import math
import jax
import jax.numpy as jnp
from jax import lax

PREDICTED_VARS = 36
MERIDIAN_NODES = 1440
L = 720
DEGREE_RANGE = 721
REALIZATIONS = 8
PARALLEL_LINES = 512
ORDERS_KEPT = 128


def draw_zonal_order_values(key, part):
    first, second = jax.random.split(key)
    inner = 1 + jax.random.permutation(first, L - 1)[:ORDERS_KEPT - 2]
    chosen = jnp.concatenate([jnp.array([0, L], dtype=jnp.int32), inner.astype(jnp.int32)])
    return jax.random.permutation(second, chosen)


def levels(rng, extent, cuts, low, largest):
    def one(axis_at, shards_of):
        steps = jax.random.uniform(jax.random.fold_in(jax.random.fold_in(rng, 6), axis_at), (shards_of,), jnp.float32, low / len(cuts), largest / len(cuts))
        return jnp.repeat(jnp.exp(steps), extent[axis_at] // shards_of).reshape((-1,) + (1,) * (len(extent) - axis_at - 1))

    gain = one(*cuts[0])
    for cut in cuts[1:]:
        gain = gain * one(*cut)
    return gain


def scatter_about(stream_key, dims, deviation, limit, cuts=(), kind=jnp.bfloat16):
    entries = jax.random.normal(stream_key, dims, jnp.float32) * deviation
    if len(cuts) > 0:
        entries = levels(stream_key, dims, cuts, -0.22, 0.18) * entries
    return jnp.clip(entries, min=-limit, max=limit).astype(kind)


def setup_inputs(seed: int = 0) -> dict:
    key_of = jax.random.split(jax.random.key(seed), 5)
    return {
        "predicted_grid": scatter_about(key_of[0], (REALIZATIONS, PREDICTED_VARS, PARALLEL_LINES, MERIDIAN_NODES), 1.0, 6.0, ((0, 4), (2, 64))),
        "verifying_coefficients": scatter_about(key_of[1], (PREDICTED_VARS, 2, ORDERS_KEPT, DEGREE_RANGE), 0.7, 5.0, ((2, 64),), jnp.float32),
        "weighted_polynomial_values": scatter_about(key_of[2], (ORDERS_KEPT, PARALLEL_LINES, DEGREE_RANGE), PARALLEL_LINES ** -0.5, 0.25, ((0, 64),)),
        "zonal_order_values": draw_zonal_order_values(jax.random.fold_in(key_of[4], 71), 0),
    }


smooth_width = 0.1

def fourier_table(zonal_order_values, meridian_node_number):
    lon_index = jnp.arange(meridian_node_number, dtype=jnp.int32)
    phases = lon_index[:, None] * zonal_order_values[None, :] % meridian_node_number
    angles = 2.0 * math.pi / meridian_node_number * phases.astype(jnp.float32)
    zonal_order_lookup = jnp.stack([jnp.cos(angles), -jnp.sin(angles)], axis=2)
    return zonal_order_lookup.reshape(meridian_node_number, -1).astype(jnp.bfloat16)

def degree_weights(zonal_order_values, degree_count):
    degrees = jnp.arange(degree_count, dtype=jnp.int32)
    factor = jnp.where(zonal_order_values == 0, 1.0, 2.0).astype(jnp.float32)
    active = (degrees[None, :] >= zonal_order_values[:, None]).astype(jnp.float32)
    return factor[:, None] * active

def soft_abs(values):
    return jnp.sqrt(values * values + smooth_width * smooth_width) - smooth_width

def soft_sign(values):
    return values / jnp.sqrt(values * values + smooth_width * smooth_width)

def reference(predicted_grid, verifying_coefficients, weighted_polynomial_values, zonal_order_values):
    realization_pile, variable_number, parallel_line_number, meridian_node_number = predicted_grid.shape
    wave_count, _, degree_count = weighted_polynomial_values.shape
    zonal_order_lookup = fourier_table(zonal_order_values, meridian_node_number)
    divisor_factor = meridian_node_number ** (-0.5)
    sphere_coefficient_sets = (jnp.dot(predicted_grid.reshape(-1, meridian_node_number), zonal_order_lookup, preferred_element_type=jnp.float32) * divisor_factor).astype(jnp.bfloat16)
    sphere_coefficient_sets = sphere_coefficient_sets.reshape(realization_pile, variable_number, parallel_line_number, wave_count, 2).transpose(3, 0, 1, 2, 4)
    slot_target = verifying_coefficients.transpose(2, 0, 1, 3)
    highest = lax.Precision.HIGHEST

    def one_slot(pieces):
        slot_spectra, basis_rows, observed, wave_number = pieces
        coeffs = jnp.einsum('mvlr,ln->vrmn', slot_spectra.astype(jnp.float32), basis_rows.astype(jnp.float32), precision=highest)
        weights = degree_weights(wave_number[None], degree_count)[0]
        gaps = coeffs[:, :, :, None, :] - coeffs[:, :, None, :, :]
        spread_abs = lax.optimization_barrier(jnp.sum(soft_abs(gaps), axis=3))
        spread_sign = lax.optimization_barrier(jnp.sum(soft_sign(gaps), axis=3))
        misses = coeffs - observed[:, :, None, :]
        scores = lax.optimization_barrier(jnp.sum(soft_abs(misses), axis=2)) / realization_pile - lax.optimization_barrier(jnp.sum(spread_abs, axis=2)) / (2 * realization_pile * realization_pile)
        probability_error_sums = lax.optimization_barrier(jnp.sum(weights * scores, axis=2)) / degree_count
        gradients = (weights * (soft_sign(misses) / realization_pile - spread_sign / (realization_pile * realization_pile))).astype(jnp.bfloat16)
        returned = jnp.einsum('vrmn,ln->mvlr', gradients.astype(jnp.float32), basis_rows.astype(jnp.float32), precision=highest).astype(jnp.bfloat16)
        return (probability_error_sums, returned)
    probability_error_sums, returned = lax.map(one_slot, (sphere_coefficient_sets, weighted_polynomial_values, slot_target, zonal_order_values))
    coefficient_error_mean = probability_error_sums.transpose(1, 2, 0)
    returned = returned.transpose(1, 2, 3, 0, 4).reshape(-1, 2 * wave_count)
    sensitivity_grid = lax.dot_general(returned, zonal_order_lookup, (((1,), (1,)), ((), ())), preferred_element_type=jnp.float32) * divisor_factor
    prediction_sensitivity = sensitivity_grid.astype(jnp.bfloat16).reshape(predicted_grid.shape)
    return (prediction_sensitivity, coefficient_error_mean)
```

```python
import functools
import math

import jax
import jax.numpy as jnp
from jax import lax
from jax.experimental import pallas as pl
from jax.experimental.pallas import tpu as pltpu
from jax.sharding import PartitionSpec as P

SMOOTH = 0.1
LANES = 128
VROWS = 40
WIDTH = 768
MEMBERS = 8
F32 = jnp.float32
BF16 = jnp.bfloat16
VMEM = pltpu.VMEM
MESH_AXES = ("ens", "lat")


def dot(a, b, dims):
    return lax.dot_general(a, b, (dims, ((), ())), preferred_element_type=F32)


def fourier_kernel(lat, z_ref, x_ref, send_ref, table_ref, x_vmem, sems):
    rows, nodes = x_vmem.shape
    chunks = [(a, min(256, rows - a)) for a in range(0, rows, 256)]
    copies = [
        pltpu.make_async_copy(x_ref.at[pl.ds(a, n)], x_vmem.at[pl.ds(a, n)], sems.at[c])
        for c, (a, n) in enumerate(chunks)
    ]
    for copy in copies:
        copy.start()
    count = send_ref.shape[0]
    waves = z_ref.shape[1]
    d = lax.broadcasted_iota(jnp.int32, (count, waves), 0)
    s = lax.broadcasted_iota(jnp.int32, (count, waves), 1)
    wanted = 2 * lax.rem(d, lat) + lax.div(d, 2 * lat)
    z = jnp.sum(jnp.where(s == wanted, z_ref[...].astype(F32), 0.0), axis=1, keepdims=True)
    dcol = lax.broadcasted_iota(jnp.int32, (count, 1), 0)
    shift = (lax.rem(lax.div(dcol, lat), 2) * (nodes // 4)).astype(F32)
    j = lax.broadcasted_iota(jnp.int32, (1, nodes), 1).astype(F32)
    step = 2.0 * math.pi / nodes
    for a in range(0, count, 32):
        p = j * z[a : a + 32] + shift[a : a + 32]
        p = p - nodes * jnp.floor(p * (1.0 / nodes))
        w = (jnp.abs(p - nodes / 2) - nodes / 4) * step
        w2 = w * w
        poly = -2.5052108e-08
        for c in (2.7557319e-06, -1.9841270e-04, 8.3333333e-03, -1.6666667e-01):
            poly = poly * w2 + c
        table_ref[a : a + 32, :] = (w + w * (w2 * poly)).astype(BF16)
    scale = nodes**-0.5
    for copy, (a, n) in zip(copies, chunks):
        copy.wait()
        spectra = dot(table_ref[...], x_vmem[a : a + n, :], ((1,), (1,))) * scale
        send_ref[:, a : a + n] = spectra.astype(BF16)
    send_ref[:, rows:] = jnp.zeros((count, send_ref.shape[1] - rows), BF16)


def crps_kernel(
    lat, ens, degrees, variables,
    z_ref, recv_ref, obs_ref, pk_ref, pl_ref, send_ref,
    turned, spectra, coeffs, grads, back, pk_vmem, pl_vmem, sems,
):
    first = pltpu.make_async_copy(pk_ref, pk_vmem, sems.at[0])
    second = pltpu.make_async_copy(pl_ref, pl_vmem, sems.at[1])
    first.start()
    second.start()
    local = MEMBERS // ens
    span = variables * 8
    pairs = ens // 2
    for k2 in range(pairs):
        rows = recv_ref[k2 * LANES : (k2 + 1) * LANES, : turned.shape[1]]
        turned[k2] = rows.astype(F32).T
    low = lax.broadcasted_iota(jnp.int32, (VROWS, LANES), 1) < lat
    for t2 in range(4):
        for m in range(local):
            for k2 in range(pairs):
                even = turned[k2, pl.ds(m * span + 2 * t2, VROWS, stride=8), :]
                odd = turned[k2, pl.ds(m * span + 2 * t2 + 1, VROWS, stride=8), :]
                into = pl.ds(t2 * LANES, LANES)
                e = 2 * k2 * local + m
                spectra[pl.ds(e * VROWS, VROWS), into] = jnp.where(low, even, pltpu.roll(odd, lat, 1))
                e = e + local
                spectra[pl.ds(e * VROWS, VROWS), into] = jnp.where(low, pltpu.roll(even, lat, 1), odd)
    first.wait()
    coeffs[...] = dot(spectra[...].astype(BF16), pk_vmem[...], ((1,), (0,)))

    zonal = z_ref[0]
    factor = jnp.where(zonal == 0, 1.0, 2.0).astype(F32)
    tiles = VROWS // 8

    def one_block(b, totals):
        lanes = pl.ds(pl.multiple_of(b * LANES, LANES), LANES)
        degree = b * LANES + lax.broadcasted_iota(jnp.int32, (8, LANES), 1)
        weight = jnp.where((degree >= zonal) & (degree < degrees), factor, 0.0)
        sums = []
        for tile in range(tiles):
            c = [coeffs[pl.ds(e * VROWS + tile * 8, 8), lanes] for e in range(MEMBERS)]
            seen = obs_ref[pl.ds(tile * 8, 8), lanes]
            slope = [None] * MEMBERS
            spread = None
            for e in range(MEMBERS - 1):
                part = None
                for f in range(e + 1, MEMBERS):
                    gap = c[e] - c[f]
                    square = gap * gap + SMOOTH * SMOOTH
                    inverse = lax.rsqrt(square)
                    sign = gap * inverse
                    root = square * inverse
                    part = root if part is None else part + root
                    slope[e] = sign if slope[e] is None else slope[e] + sign
                    slope[f] = -sign if slope[f] is None else slope[f] - sign
                part = part - SMOOTH * (MEMBERS - 1 - e)
                spread = part if spread is None else spread + part
            miss = None
            for e in range(MEMBERS):
                gap = c[e] - seen
                square = gap * gap + SMOOTH * SMOOTH
                inverse = lax.rsqrt(square)
                root = square * inverse
                miss = root if miss is None else miss + root
                grad = weight * (gap * inverse * (1 / MEMBERS) - slope[e] * (1 / MEMBERS**2))
                grads[pl.ds(e * VROWS + tile * 8, 8), lanes] = grad.astype(BF16)
            miss = miss - SMOOTH * MEMBERS
            score = miss * (1 / MEMBERS) - spread * (1 / MEMBERS**2)
            sums.append(totals[tile] + weight * score)
        return tuple(sums)

    blocks = coeffs.shape[1] // LANES
    zero = jnp.zeros((8, LANES), F32)
    totals = lax.fori_loop(0, blocks, one_block, (zero,) * tiles)

    second.wait()
    returned = dot(grads[...], pl_vmem[...], ((1,), (0,)))
    for m in range(local):
        for t2 in range(4):
            for k2 in range(pairs):
                e = 2 * k2 * local + m
                even = returned[e * VROWS : (e + 1) * VROWS, t2 * LANES : (t2 + 1) * LANES]
                e = e + local
                odd = returned[e * VROWS : (e + 1) * VROWS, t2 * LANES : (t2 + 1) * LANES]
                row = m * span + 2 * t2
                back[k2, pl.ds(row, VROWS, stride=8), :] = jnp.where(low, even, pltpu.roll(odd, lat, 1))
                back[k2, pl.ds(row + 1, VROWS, stride=8), :] = jnp.where(low, pltpu.roll(even, lat, 1), odd)
    base = back.shape[1] - LANES
    for tile in range(tiles):
        rest = jnp.sum(totals[tile], axis=1, keepdims=True) * (1.0 / degrees)
        for term in range(3):
            piece = rest.astype(BF16).astype(F32)
            rest = rest - piece
            for k2 in range(pairs):
                spot = pl.ds(base + term * VROWS + tile * 8, 8)
                back[k2, spot, :] = jnp.broadcast_to(piece, (8, LANES))
    for k2 in range(pairs):
        back[k2, base + 3 * VROWS :, :] = jnp.zeros((LANES - 3 * VROWS, LANES), F32)
        send_ref[k2 * LANES : (k2 + 1) * LANES, :] = back[k2].T.astype(BF16)


def grid_kernel(lat, ens, variables, at_ref, recv_ref, table_ref, out_ref, score_ref, block, sems):
    rows, nodes = out_ref.shape
    scale = nodes**-0.5
    copies = []
    for c, a in enumerate(range(0, rows, LANES)):
        n = min(LANES, rows - a)
        part = dot(recv_ref[:, a : a + n], table_ref[...], ((0,), (0,))) * scale
        block[a : a + n, :] = part.astype(BF16)
        copy = pltpu.make_async_copy(block.at[pl.ds(a, n)], out_ref.at[pl.ds(a, n)], sems.at[c])
        copy.start()
        copies.append(copy)
    base = recv_ref.shape[1] - LANES
    mine = lax.broadcasted_iota(jnp.int32, (lat, LANES), 0) == at_ref[0]
    for k in range(ens):
        terms = recv_ref[k * lat : (k + 1) * lat, base : base + LANES].astype(F32)
        terms = jnp.sum(jnp.where(mine, terms, 0.0), axis=0, keepdims=True)
        total = terms + pltpu.roll(terms, LANES - VROWS, 1) + pltpu.roll(terms, LANES - 2 * VROWS, 1)
        score_ref[k % 2, k // 2 : k // 2 + 1, :] = total[:, :variables]
    for copy in copies:
        copy.wait()


def exchange(values):
    count, width = values.shape
    values = values.reshape(count, 2, width // 2)
    values = lax.all_to_all(values, MESH_AXES, 0, 0, tiled=True)
    return values.reshape(count, width)


def body(predicted_grid, verifying_coefficients, weighted_polynomial_values, zonal_order_values):
    local, variables, lines, nodes = predicted_grid.shape
    _, all_lines, degrees = weighted_polynomial_values.shape
    lat = lax.axis_size("lat")
    ens = lax.axis_size("ens")
    count = lat * ens
    rows = local * variables * lines
    padded = -(-degrees // LANES) * LANES
    whole = pl.BlockSpec(memory_space=VMEM)
    scalar = pl.BlockSpec(memory_space=pltpu.SMEM)
    anywhere = pl.BlockSpec(memory_space=pl.ANY)
    at_lat = lax.axis_index("lat")
    at_ens = lax.axis_index("ens")
    slot = at_ens // 2
    part = at_ens % 2

    send, table = pl.pallas_call(
        functools.partial(fourier_kernel, lat),
        name="fourier",
        in_specs=[whole, anywhere],
        out_specs=[whole, whole],
        out_shape=[
            jax.ShapeDtypeStruct((count, WIDTH), BF16),
            jax.ShapeDtypeStruct((count, nodes), BF16),
        ],
        scratch_shapes=[VMEM((rows, nodes), BF16), pltpu.SemaphoreType.DMA((3,))],
    )(zonal_order_values.reshape(1, -1), predicted_grid.reshape(rows, nodes))
    recv = exchange(send)

    basis = lax.dynamic_index_in_dim(weighted_polynomial_values, slot, 0, False)
    basis = basis.reshape(lat, lines, degrees).transpose(1, 0, 2).reshape(all_lines, degrees)
    basis = jnp.pad(basis, ((0, 0), (0, padded - degrees)))
    observed = lax.dynamic_index_in_dim(verifying_coefficients, part, 1, False)
    observed = lax.dynamic_index_in_dim(observed, slot, 1, False)
    observed = jnp.pad(observed, ((0, VROWS - variables), (0, padded - degrees)))
    own_wave = lax.dynamic_slice_in_dim(zonal_order_values, 2 * at_lat + slot, 1)

    send = pl.pallas_call(
        functools.partial(crps_kernel, lat, ens, degrees, variables),
        name="crps",
        in_specs=[scalar, whole, whole, anywhere, anywhere],
        out_specs=whole,
        out_shape=jax.ShapeDtypeStruct((count, WIDTH), BF16),
        scratch_shapes=[
            VMEM((ens // 2, 5 * LANES, LANES), F32),
            VMEM((MEMBERS * VROWS, all_lines), F32),
            VMEM((MEMBERS * VROWS, padded), F32),
            VMEM((MEMBERS * VROWS, padded), BF16),
            VMEM((ens // 2, WIDTH, LANES), F32),
            VMEM((all_lines, padded), BF16),
            VMEM((padded, all_lines), BF16),
            pltpu.SemaphoreType.DMA((2,)),
        ],
    )(own_wave, recv, observed, basis, basis.T)
    recv = exchange(send)

    sensitivity, scores = pl.pallas_call(
        functools.partial(grid_kernel, lat, ens, variables),
        name="grid",
        in_specs=[scalar, whole, whole],
        out_specs=[anywhere, whole],
        out_shape=[
            jax.ShapeDtypeStruct((rows, nodes), BF16),
            jax.ShapeDtypeStruct((2, 2, variables), F32),
        ],
        scratch_shapes=[VMEM((rows, nodes), BF16), pltpu.SemaphoreType.DMA((5,))],
    )(at_lat.reshape(1), recv, table)
    return sensitivity.reshape(predicted_grid.shape), scores.transpose(2, 0, 1)


def solution(mesh):
    placed = (P("ens", None, "lat", None), P(None, None, "lat", None), P("lat", None, None), P())
    return jax.shard_map(
        body,
        mesh=mesh,
        in_specs=placed,
        out_specs=(P("ens", None, "lat", None), P(None, None, "lat")),
        check_vma=False,
    )
```

```python
import functools
import math

import jax
import jax.numpy as jnp
from jax import lax
from jax.experimental import pallas as pl
from jax.experimental.pallas import tpu as pltpu
from jax.sharding import PartitionSpec as P

SMOOTH = 0.1
LANES = 128
VROWS = 40
WIDTH = 384
MEMBERS = 8
F32 = jnp.float32
BF16 = jnp.bfloat16
VMEM = pltpu.VMEM
PARAMS = pltpu.CompilerParams(vmem_limit_bytes=16 * 1024 * 1024)
MESH_AXES = ("ens", "lat")


def dot(a, b, dims):
    return lax.dot_general(a, b, (dims, ((), ())), preferred_element_type=F32)


def fourier_kernel(lat, z_far, x_ref, send_ref, table_far, z_ref, x_vmem, table_ref, sems):
    local, width, nodes = x_vmem.shape
    span = x_ref.shape[1]
    copies = [
        pltpu.make_async_copy(x_ref.at[m], x_vmem.at[m, pl.ds(0, span)], sems.at[m]) for m in range(local)
    ]
    waves = pltpu.make_async_copy(z_far, z_ref, sems.at[local + 1])
    waves.start()
    for copy in copies:
        copy.start()
    for m in range(local):
        x_vmem[m, span:, :] = jnp.zeros((width - span, nodes), BF16)
    count = send_ref.shape[0]
    shape = (count, z_ref.shape[1])
    d = lax.broadcasted_iota(jnp.int32, shape, 0)
    s = lax.broadcasted_iota(jnp.int32, shape, 1)
    wanted = 2 * lax.rem(d, lat) + lax.div(d, 2 * lat)
    waves.wait()
    z = jnp.sum(jnp.where(s == wanted, z_ref[...].astype(F32), 0.0), axis=1, keepdims=True)
    dcol = lax.broadcasted_iota(jnp.int32, (count, 1), 0)
    shift = (lax.rem(lax.div(dcol, lat), 2) * (nodes // 4)).astype(F32)
    j = lax.broadcasted_iota(jnp.int32, (1, nodes), 1).astype(F32)
    step = 2.0 * math.pi / nodes
    for a in range(0, count, 32):
        p = j * z[a : a + 32] + shift[a : a + 32]
        p = p - nodes * jnp.floor(p * (1.0 / nodes))
        w = (jnp.abs(p - nodes / 2) - nodes / 4) * step
        w2 = w * w
        poly = -2.5052108e-08
        for c in (2.7557319e-06, -1.9841270e-04, 8.3333333e-03, -1.6666667e-01):
            poly = poly * w2 + c
        table_ref[a : a + 32, :] = (w + w * (w2 * poly)).astype(BF16)
    scale = nodes**-0.5
    keep = pltpu.make_async_copy(table_ref, table_far, sems.at[local])
    keep.start()
    for m, copy in enumerate(copies):
        copy.wait()
        spectra = dot(table_ref[...], x_vmem[m], ((1,), (1,))) * scale
        send_ref[:, m, :] = spectra.astype(BF16)
    keep.wait()


def basis_kernel(lat, where_ref, p_ref, v_ref, pk_ref, pl_ref, obs_ref, p_vmem, v_vmem, mine, sems):
    slot = where_ref[0]
    first = pltpu.make_async_copy(p_ref, p_vmem, sems.at[0])
    second = pltpu.make_async_copy(v_ref.at[:, where_ref[1]], v_vmem, sems.at[1])
    first.start()
    second.start()
    degrees, _, lines = p_vmem.shape
    first.wait()
    step = 16

    def pick(start, size):
        both = p_vmem[pl.ds(start, size)].astype(F32)
        chosen = jnp.where(slot == 0, both[:, 0, :], both[:, 1, :])
        mine[pl.ds(start, size), :] = chosen.astype(BF16)

    def one(i, carry):
        pick(pl.multiple_of(i * step, step), step)
        return carry

    lax.fori_loop(0, degrees // step, one, 0)
    rest = degrees % step
    if rest:
        pick(degrees - rest, rest)
    rows = lines // lat
    source = lax.broadcasted_iota(jnp.int32, (lines, lines), 0)
    target = lax.broadcasted_iota(jnp.int32, (lines, lines), 1)
    order = source == rows * lax.rem(target, lat) + lax.div(target, lat)
    turned = dot(mine[...], order.astype(F32).astype(BF16), ((1,), (0,)))
    pl_ref[...] = turned.astype(BF16)
    pk_ref[...] = turned.T.astype(BF16)
    second.wait()
    seen = v_vmem[...]
    obs_ref[...] = jnp.zeros(obs_ref.shape, F32)
    obs_ref[: seen.shape[0], :degrees] = jnp.where(slot == 0, seen[:, 0, :], seen[:, 1, :])


def crps_kernel(
    lat, ens, degrees, variables,
    z_ref, recv_ref, obs_far, pk_far, pl_far, send_ref,
    turned, spectra, coeffs, grads, back, obs_ref, pk_ref, pl_ref, sems,
):
    copies = [
        pltpu.make_async_copy(far, near, sems.at[c])
        for c, (far, near) in enumerate(((pk_far, pk_ref), (obs_far, obs_ref), (pl_far, pl_ref)))
    ]
    for copy in copies:
        copy.start()
    local = MEMBERS // ens
    pairs = ens // 2
    for m in range(local):
        for k2 in range(pairs):
            rows = recv_ref[k2 * LANES : (k2 + 1) * LANES, m, :]
            turned[m, k2] = rows.astype(F32).T
    low = lax.broadcasted_iota(jnp.int32, (VROWS, LANES), 1) < lat
    for t2 in range(4):
        for m in range(local):
            for k2 in range(pairs):
                even = turned[m, k2, pl.ds(2 * t2, VROWS, stride=8), :]
                odd = turned[m, k2, pl.ds(2 * t2 + 1, VROWS, stride=8), :]
                into = pl.ds(t2 * LANES, LANES)
                e = 2 * k2 * local + m
                spectra[pl.ds(e * VROWS, VROWS), into] = jnp.where(low, even, pltpu.roll(odd, lat, 1))
                e = e + local
                spectra[pl.ds(e * VROWS, VROWS), into] = jnp.where(low, pltpu.roll(even, lat, 1), odd)
    copies[0].wait()
    coeffs[:, :degrees] = dot(spectra[...].astype(BF16), pk_ref[...], ((1,), (0,)))

    copies[1].wait()
    zonal = z_ref[0]
    factor = jnp.where(zonal == 0, 1.0, 2.0).astype(F32)
    tiles = VROWS // 8

    def one_block(b, totals):
        lanes = pl.ds(pl.multiple_of(b * LANES, LANES), LANES)
        degree = b * LANES + lax.broadcasted_iota(jnp.int32, (8, LANES), 1)
        active = (degree >= zonal) & (degree < degrees)
        sums = []
        for tile in range(tiles):
            c = [coeffs[pl.ds(e * VROWS + tile * 8, 8), lanes] for e in range(MEMBERS)]
            seen = obs_ref[pl.ds(tile * 8, 8), lanes]
            slope = [None] * MEMBERS
            spread = None
            for e in range(MEMBERS - 1):
                part = None
                for f in range(e + 1, MEMBERS):
                    gap = c[e] - c[f]
                    square = gap * gap + SMOOTH * SMOOTH
                    inverse = lax.rsqrt(square)
                    sign = gap * inverse
                    root = square * inverse
                    part = root if part is None else part + root
                    slope[e] = sign if slope[e] is None else slope[e] + sign
                    slope[f] = -sign if slope[f] is None else slope[f] - sign
                part = part - SMOOTH * (MEMBERS - 1 - e)
                spread = part if spread is None else spread + part
            miss = None
            for e in range(MEMBERS):
                gap = c[e] - seen
                square = gap * gap + SMOOTH * SMOOTH
                inverse = lax.rsqrt(square)
                root = square * inverse
                miss = root if miss is None else miss + root
                grad = factor * (gap * inverse * (1 / MEMBERS) - slope[e] * (1 / MEMBERS**2))
                grad = jnp.where(active, grad, 0.0)
                grads[pl.ds(e * VROWS + tile * 8, 8), lanes] = grad.astype(BF16)
            miss = miss - SMOOTH * MEMBERS
            score = miss * (1 / MEMBERS) - spread * (1 / MEMBERS**2)
            sums.append(totals[tile] + jnp.where(active, factor * score, 0.0))
        return tuple(sums)

    blocks = coeffs.shape[1] // LANES
    zero = jnp.zeros((8, LANES), F32)
    totals = lax.fori_loop(0, blocks, one_block, (zero,) * tiles)

    copies[2].wait()
    returned = dot(grads[:, :degrees], pl_ref[...], ((1,), (0,)))
    for m in range(local):
        for t2 in range(4):
            for k2 in range(pairs):
                e = 2 * k2 * local + m
                even = returned[e * VROWS : (e + 1) * VROWS, t2 * LANES : (t2 + 1) * LANES]
                e = e + local
                odd = returned[e * VROWS : (e + 1) * VROWS, t2 * LANES : (t2 + 1) * LANES]
                row = 2 * t2
                back[m, k2, pl.ds(row, VROWS, stride=8), :] = jnp.where(low, even, pltpu.roll(odd, lat, 1))
                back[m, k2, pl.ds(row + 1, VROWS, stride=8), :] = jnp.where(low, pltpu.roll(even, lat, 1), odd)
    span = variables * 8
    for tile in range(tiles):
        rest = jnp.sum(totals[tile], axis=1, keepdims=True) * (1.0 / degrees)
        for m, at in ((0, span), (0, span + VROWS), (1, span)):
            piece = rest.astype(BF16).astype(F32)
            rest = rest - piece
            for k2 in range(pairs):
                back[m, k2, pl.ds(at + tile * 8, 8), :] = jnp.broadcast_to(piece, (8, LANES))
    for m in range(local):
        used = span + VROWS * (2 - m)
        for k2 in range(pairs):
            back[m, k2, used:, :] = jnp.zeros((WIDTH - used, LANES), F32)
            send_ref[k2 * LANES : (k2 + 1) * LANES, m, :] = back[m, k2].T.astype(BF16)


def grid_kernel(lat, ens, variables, at_ref, recv_ref, table_far, out_ref, score_ref, block, table_ref, sems):
    load = pltpu.make_async_copy(table_far, table_ref, sems.at[6])
    load.start()
    local, span, nodes = out_ref.shape
    scale = nodes**-0.5
    copies = []
    for m in range(local):
        turned = recv_ref[:, m, :].astype(F32).T.astype(BF16)
        if m == 0:
            load.wait()
        for a in range(0, span, LANES):
            n = min(LANES, span - a)
            part = dot(turned[a : a + n, :], table_ref[...], ((1,), (0,))) * scale
            block[m, a : a + n, :] = part.astype(BF16)
            copy = pltpu.make_async_copy(
                block.at[m, pl.ds(a, n)], out_ref.at[m, pl.ds(a, n)], sems.at[len(copies)]
            )
            copy.start()
            copies.append(copy)
    base = WIDTH - LANES
    mine = lax.broadcasted_iota(jnp.int32, (lat, LANES), 0) == at_ref[0]
    for k in range(ens):
        terms = [
            jnp.sum(
                jnp.where(mine, recv_ref[k * lat : (k + 1) * lat, m, base:].astype(F32), 0.0),
                axis=0, keepdims=True,
            )
            for m in range(2)
        ]
        total = terms[0] + pltpu.roll(terms[0], LANES - VROWS, 1) + terms[1]
        total = pltpu.roll(total, LANES - (span - base), 1)
        score_ref[k % 2, k // 2 : k // 2 + 1, :] = total[:, :variables]
    for copy in copies:
        copy.wait()


def far_of(*arrays):
    return [pltpu.with_memory_space_constraint(a, pltpu.HBM) for a in arrays]


def exchange(values):
    return lax.all_to_all(values, MESH_AXES, 0, 0, tiled=True)


def body(predicted_grid, verifying_coefficients, weighted_polynomial_values, zonal_order_values):
    local, variables, lines, nodes = predicted_grid.shape
    slots, all_lines, degrees = weighted_polynomial_values.shape
    lat = lax.axis_size("lat")
    ens = lax.axis_size("ens")
    count = lat * ens
    span = variables * lines
    padded = -(-degrees // LANES) * LANES
    whole = pl.BlockSpec(memory_space=VMEM)
    scalar = pl.BlockSpec(memory_space=pltpu.SMEM)
    far = pl.BlockSpec(memory_space=pltpu.HBM)
    at_lat = lax.axis_index("lat")
    at_ens = lax.axis_index("ens")
    slot = at_ens // 2
    sent = jax.ShapeDtypeStruct((count, local, WIDTH), BF16)

    send, table = pl.pallas_call(
        functools.partial(fourier_kernel, lat),
        name="fourier",
        compiler_params=PARAMS,
        in_specs=[far, far],
        out_specs=[whole, far],
        out_shape=[sent, pltpu.HBM((count, nodes), BF16)],
        scratch_shapes=[
            VMEM((1, zonal_order_values.shape[0]), jnp.int32),
            VMEM((local, WIDTH, nodes), BF16),
            VMEM((count, nodes), BF16),
            pltpu.SemaphoreType.DMA((4,)),
        ],
    )(*far_of(zonal_order_values.reshape(1, -1), predicted_grid.reshape(local, span, nodes)))
    recv = exchange(send)

    by_line, by_degree, observed = pl.pallas_call(
        functools.partial(basis_kernel, lat),
        name="basis",
        compiler_params=PARAMS,
        in_specs=[scalar, far, far],
        out_specs=[whole, whole, whole],
        out_shape=[
            pltpu.HBM((all_lines, degrees), BF16),
            pltpu.HBM((degrees, all_lines), BF16),
            pltpu.HBM((VROWS, padded), F32),
        ],
        scratch_shapes=[
            VMEM((degrees, slots, all_lines), BF16),
            VMEM((variables, slots, degrees), F32),
            VMEM((degrees, all_lines), BF16),
            pltpu.SemaphoreType.DMA((2,)),
        ],
        cost_estimate=pl.CostEstimate(flops=2 * degrees * all_lines**2, bytes_accessed=4_000_000, transcendentals=0),
    )(
        jnp.stack([slot, at_ens % 2]),
        *far_of(weighted_polynomial_values.transpose(2, 0, 1), verifying_coefficients),
    )
    own_wave = lax.dynamic_slice_in_dim(zonal_order_values, 2 * at_lat + slot, 1)

    send = pl.pallas_call(
        functools.partial(crps_kernel, lat, ens, degrees, variables),
        name="crps",
        compiler_params=PARAMS,
        in_specs=[scalar, whole, far, far, far],
        out_specs=whole,
        out_shape=sent,
        scratch_shapes=[
            VMEM((local, ens // 2, WIDTH, LANES), F32),
            VMEM((MEMBERS * VROWS, all_lines), F32),
            VMEM((MEMBERS * VROWS, padded), F32),
            VMEM((MEMBERS * VROWS, padded), BF16),
            VMEM((local, ens // 2, WIDTH, LANES), F32),
            VMEM((VROWS, padded), F32),
            VMEM((all_lines, degrees), BF16),
            VMEM((degrees, all_lines), BF16),
            pltpu.SemaphoreType.DMA((3,)),
        ],
    )(own_wave, recv, *far_of(observed, by_line, by_degree))
    recv = exchange(send)

    sensitivity, scores = pl.pallas_call(
        functools.partial(grid_kernel, lat, ens, variables),
        name="grid",
        compiler_params=PARAMS,
        in_specs=[scalar, whole, far],
        out_specs=[far, whole],
        out_shape=[
            jax.ShapeDtypeStruct((local, span, nodes), BF16),
            jax.ShapeDtypeStruct((2, 2, variables), F32),
        ],
        scratch_shapes=[
            VMEM((local, span, nodes), BF16),
            VMEM((count, nodes), BF16),
            pltpu.SemaphoreType.DMA((7,)),
        ],
    )(at_lat.reshape(1), recv, *far_of(table))
    return sensitivity.reshape(predicted_grid.shape), scores.transpose(2, 0, 1)


def solution(mesh):
    placed = (P("ens", None, "lat", None), P(None, None, "lat", None), P("lat", None, None), P())
    return jax.shard_map(
        body,
        mesh=mesh,
        in_specs=placed,
        out_specs=(P("ens", None, "lat", None), P(None, None, "lat")),
        check_vma=False,
    )
```

```python
import functools
import math

import jax
import jax.numpy as jnp
from jax import lax
from jax.experimental import pallas as pl
from jax.experimental.pallas import tpu as pltpu
from jax.sharding import PartitionSpec as P

SMOOTH = 0.1
LANES = 128
VROWS = 40
WIDTH = 384
MEMBERS = 8
F32 = jnp.float32
BF16 = jnp.bfloat16
VMEM = pltpu.VMEM
PARAMS = pltpu.CompilerParams(vmem_limit_bytes=16 * 1024 * 1024)
MESH_AXES = ("ens", "lat")


def dot(a, b, dims):
    return lax.dot_general(a, b, (dims, ((), ())), preferred_element_type=F32)


def fourier_kernel(lat, z_far, x_ref, send_ref, table_far, z_ref, x_vmem, table_ref, sems):
    local, width, nodes = x_vmem.shape
    span = x_ref.shape[1]
    copies = [
        pltpu.make_async_copy(x_ref.at[m], x_vmem.at[m, pl.ds(0, span)], sems.at[m]) for m in range(local)
    ]
    waves = pltpu.make_async_copy(z_far, z_ref, sems.at[local + 1])
    waves.start()
    for copy in copies:
        copy.start()
    for m in range(local):
        x_vmem[m, span:, :] = jnp.zeros((width - span, nodes), BF16)
    count = send_ref.shape[0]
    shape = (count, z_ref.shape[1])
    d = lax.broadcasted_iota(jnp.int32, shape, 0)
    s = lax.broadcasted_iota(jnp.int32, shape, 1)
    wanted = 2 * lax.rem(d, lat) + lax.div(d, 2 * lat)
    waves.wait()
    z = jnp.sum(jnp.where(s == wanted, z_ref[...].astype(F32), 0.0), axis=1, keepdims=True)
    step = 2.0 * math.pi / nodes

    def cosine(p):
        p = p - nodes * jnp.floor(p * (1.0 / nodes))
        w = (jnp.abs(p - nodes / 2) - nodes / 4) * step
        w2 = w * w
        poly = -2.5052108e-08
        for c in (2.7557319e-06, -1.9841270e-04, 8.3333333e-03, -1.6666667e-01):
            poly = poly * w2 + c
        return w + w * (w2 * poly)

    j = lax.broadcasted_iota(jnp.int32, (1, LANES), 1).astype(F32)
    turn = nodes // 4
    for half in range(count // (2 * lat)):
        for a in range(0, lat, 16):
            at = 2 * lat * half + a
            wave = jnp.broadcast_to(z[at : at + 16], (16, LANES))
            phase = wave * j
            real, imag = cosine(phase), cosine(phase + turn)
            ahead = wave * LANES
            keep_part, swap_part = cosine(ahead), cosine(ahead + turn)
            for b in range(0, nodes, LANES):
                n = min(LANES, nodes - b)
                table_ref[at : at + 16, b : b + n] = real[:, :n].astype(BF16)
                table_ref[at + lat : at + lat + 16, b : b + n] = imag[:, :n].astype(BF16)
                real, imag = (
                    real * keep_part - imag * swap_part,
                    imag * keep_part + real * swap_part,
                )
    scale = nodes**-0.5
    keep = pltpu.make_async_copy(table_ref, table_far, sems.at[local])
    keep.start()
    for m, copy in enumerate(copies):
        copy.wait()
        spectra = dot(table_ref[...], x_vmem[m], ((1,), (1,))) * scale
        send_ref[:, m, :] = spectra.astype(BF16)
    keep.wait()


def basis_kernel(lat, where_ref, p_ref, v_ref, basis_ref, obs_ref, p_vmem, v_vmem, mine, sems):
    slot = where_ref[0]
    first = pltpu.make_async_copy(p_ref, p_vmem, sems.at[0])
    second = pltpu.make_async_copy(v_ref.at[:, where_ref[1]], v_vmem, sems.at[1])
    first.start()
    second.start()
    degrees, _, lines = p_vmem.shape
    first.wait()
    step = 16

    def pick(start, size):
        both = p_vmem[pl.ds(start, size)].astype(F32)
        chosen = jnp.where(slot == 0, both[:, 0, :], both[:, 1, :])
        mine[pl.ds(start, size), :] = chosen.astype(BF16)

    def one(i, carry):
        pick(pl.multiple_of(i * step, step), step)
        return carry

    lax.fori_loop(0, degrees // step, one, 0)
    rest = degrees % step
    if rest:
        pick(degrees - rest, rest)
    rows = lines // lat
    source = lax.broadcasted_iota(jnp.int32, (lines, lines), 0)
    target = lax.broadcasted_iota(jnp.int32, (lines, lines), 1)
    order = source == rows * lax.rem(target, lat) + lax.div(target, lat)
    turned = dot(mine[...], order.astype(F32).astype(BF16), ((1,), (0,)))
    basis_ref[...] = turned.astype(BF16)
    second.wait()
    seen = v_vmem[...]
    obs_ref[...] = jnp.zeros(obs_ref.shape, F32)
    obs_ref[: seen.shape[0], :degrees] = jnp.where(slot == 0, seen[:, 0, :], seen[:, 1, :])


def crps_kernel(
    lat, ens, degrees, variables,
    z_ref, recv_ref, obs_ref, basis_ref, send_ref,
    turned, spectra, coeffs, grads, back,
):
    local = MEMBERS // ens
    pairs = ens // 2
    for m in range(local):
        for k2 in range(pairs):
            rows = recv_ref[k2 * LANES : (k2 + 1) * LANES, m, :]
            turned[m, k2] = rows.astype(F32).T
    low = lax.broadcasted_iota(jnp.int32, (VROWS, LANES), 1) < lat
    for t2 in range(4):
        for m in range(local):
            for k2 in range(pairs):
                even = turned[m, k2, pl.ds(2 * t2, VROWS, stride=8), :]
                odd = turned[m, k2, pl.ds(2 * t2 + 1, VROWS, stride=8), :]
                into = pl.ds(t2 * LANES, LANES)
                e = 2 * k2 * local + m
                spectra[pl.ds(e * VROWS, VROWS), into] = jnp.where(low, even, pltpu.roll(odd, lat, 1))
                e = e + local
                spectra[pl.ds(e * VROWS, VROWS), into] = jnp.where(low, pltpu.roll(even, lat, 1), odd)
    coeffs[:, :degrees] = dot(spectra[...].astype(BF16), basis_ref[...], ((1,), (1,)))

    zonal = z_ref[0]
    factor = jnp.where(zonal == 0, 1.0, 2.0).astype(F32)
    tiles = VROWS // 8

    def one_block(b, totals):
        lanes = pl.ds(pl.multiple_of(b * LANES, LANES), LANES)
        degree = b * LANES + lax.broadcasted_iota(jnp.int32, (8, LANES), 1)
        active = (degree >= zonal) & (degree < degrees)
        sums = []
        for tile in range(tiles):
            c = [coeffs[pl.ds(e * VROWS + tile * 8, 8), lanes] for e in range(MEMBERS)]
            seen = obs_ref[pl.ds(tile * 8, 8), lanes]
            slope = [None] * MEMBERS
            spread = None
            for e in range(MEMBERS - 1):
                part = None
                for f in range(e + 1, MEMBERS):
                    gap = c[e] - c[f]
                    square = gap * gap + SMOOTH * SMOOTH
                    inverse = lax.rsqrt(square)
                    sign = gap * inverse
                    root = square * inverse
                    part = root if part is None else part + root
                    slope[e] = sign if slope[e] is None else slope[e] + sign
                    slope[f] = -sign if slope[f] is None else slope[f] - sign
                part = part - SMOOTH * (MEMBERS - 1 - e)
                spread = part if spread is None else spread + part
            miss = None
            for e in range(MEMBERS):
                gap = c[e] - seen
                square = gap * gap + SMOOTH * SMOOTH
                inverse = lax.rsqrt(square)
                root = square * inverse
                miss = root if miss is None else miss + root
                grad = factor * (gap * inverse * (1 / MEMBERS) - slope[e] * (1 / MEMBERS**2))
                grad = jnp.where(active, grad, 0.0)
                grads[pl.ds(e * VROWS + tile * 8, 8), lanes] = grad.astype(BF16)
            miss = miss - SMOOTH * MEMBERS
            score = miss * (1 / MEMBERS) - spread * (1 / MEMBERS**2)
            sums.append(totals[tile] + jnp.where(active, factor * score, 0.0))
        return tuple(sums)

    blocks = coeffs.shape[1] // LANES
    zero = jnp.zeros((8, LANES), F32)
    totals = lax.fori_loop(0, blocks, one_block, (zero,) * tiles)

    returned = dot(grads[:, :degrees], basis_ref[...], ((1,), (0,)))
    for m in range(local):
        for t2 in range(4):
            for k2 in range(pairs):
                e = 2 * k2 * local + m
                even = returned[e * VROWS : (e + 1) * VROWS, t2 * LANES : (t2 + 1) * LANES]
                e = e + local
                odd = returned[e * VROWS : (e + 1) * VROWS, t2 * LANES : (t2 + 1) * LANES]
                row = 2 * t2
                back[m, k2, pl.ds(row, VROWS, stride=8), :] = jnp.where(low, even, pltpu.roll(odd, lat, 1))
                back[m, k2, pl.ds(row + 1, VROWS, stride=8), :] = jnp.where(low, pltpu.roll(even, lat, 1), odd)
    span = variables * 8
    for tile in range(tiles):
        rest = jnp.sum(totals[tile], axis=1, keepdims=True) * (1.0 / degrees)
        for m, at in ((0, span), (0, span + VROWS), (1, span)):
            piece = rest.astype(BF16).astype(F32)
            rest = rest - piece
            for k2 in range(pairs):
                back[m, k2, pl.ds(at + tile * 8, 8), :] = jnp.broadcast_to(piece, (8, LANES))
    for m in range(local):
        used = span + VROWS * (2 - m)
        for k2 in range(pairs):
            back[m, k2, used:, :] = jnp.zeros((WIDTH - used, LANES), F32)
            send_ref[k2 * LANES : (k2 + 1) * LANES, m, :] = back[m, k2].T.astype(BF16)


def grid_kernel(lat, ens, variables, at_ref, recv_ref, table_ref, out_ref, score_ref, block, sems):
    local, span, nodes = out_ref.shape
    scale = nodes**-0.5
    copies = []
    for m in range(local):
        turned = recv_ref[:, m, :].astype(F32).T.astype(BF16)
        for a in range(0, span, LANES):
            n = min(LANES, span - a)
            part = dot(turned[a : a + n, :], table_ref[...], ((1,), (0,))) * scale
            block[m, a : a + n, :] = part.astype(BF16)
            copy = pltpu.make_async_copy(
                block.at[m, pl.ds(a, n)], out_ref.at[m, pl.ds(a, n)], sems.at[len(copies)]
            )
            copy.start()
            copies.append(copy)
    base = WIDTH - LANES
    mine = lax.broadcasted_iota(jnp.int32, (lat, LANES), 0) == at_ref[0]
    for k in range(ens):
        terms = [
            jnp.sum(
                jnp.where(mine, recv_ref[k * lat : (k + 1) * lat, m, base:].astype(F32), 0.0),
                axis=0, keepdims=True,
            )
            for m in range(2)
        ]
        total = terms[0] + pltpu.roll(terms[0], LANES - VROWS, 1) + terms[1]
        total = pltpu.roll(total, LANES - (span - base), 1)
        score_ref[k % 2, k // 2 : k // 2 + 1, :] = total[:, :variables]
    for copy in copies:
        copy.wait()


def far_of(*arrays):
    return [pltpu.with_memory_space_constraint(a, pltpu.HBM) for a in arrays]


def exchange(values):
    return lax.all_to_all(values, MESH_AXES, 0, 0, tiled=True)


def body(predicted_grid, verifying_coefficients, weighted_polynomial_values, zonal_order_values):
    local, variables, lines, nodes = predicted_grid.shape
    slots, all_lines, degrees = weighted_polynomial_values.shape
    lat = lax.axis_size("lat")
    ens = lax.axis_size("ens")
    count = lat * ens
    span = variables * lines
    padded = -(-degrees // LANES) * LANES
    whole = pl.BlockSpec(memory_space=VMEM)
    scalar = pl.BlockSpec(memory_space=pltpu.SMEM)
    far = pl.BlockSpec(memory_space=pltpu.HBM)
    at_lat = lax.axis_index("lat")
    at_ens = lax.axis_index("ens")
    slot = at_ens // 2
    sent = jax.ShapeDtypeStruct((count, local, WIDTH), BF16)

    send, table = pl.pallas_call(
        functools.partial(fourier_kernel, lat),
        name="fourier",
        compiler_params=PARAMS,
        in_specs=[far, far],
        out_specs=[whole, far],
        out_shape=[sent, pltpu.HBM((count, nodes), BF16)],
        scratch_shapes=[
            VMEM((1, zonal_order_values.shape[0]), jnp.int32),
            VMEM((local, WIDTH, nodes), BF16),
            VMEM((count, nodes), BF16),
            pltpu.SemaphoreType.DMA((4,)),
        ],
    )(*far_of(zonal_order_values.reshape(1, -1), predicted_grid.reshape(local, span, nodes)))
    recv = exchange(send)

    basis, observed = pl.pallas_call(
        functools.partial(basis_kernel, lat),
        name="basis",
        compiler_params=PARAMS,
        in_specs=[scalar, far, far],
        out_specs=[whole, whole],
        out_shape=[
            jax.ShapeDtypeStruct((degrees, all_lines), BF16),
            jax.ShapeDtypeStruct((VROWS, padded), F32),
        ],
        scratch_shapes=[
            VMEM((degrees, slots, all_lines), BF16),
            VMEM((variables, slots, degrees), F32),
            VMEM((degrees, all_lines), BF16),
            pltpu.SemaphoreType.DMA((2,)),
        ],
        cost_estimate=pl.CostEstimate(flops=2 * degrees * all_lines**2, bytes_accessed=4_000_000, transcendentals=0),
    )(
        jnp.stack([slot, at_ens % 2]),
        *far_of(weighted_polynomial_values.transpose(2, 0, 1), verifying_coefficients),
    )
    own_wave = lax.dynamic_slice_in_dim(zonal_order_values, 2 * at_lat + slot, 1)

    send = pl.pallas_call(
        functools.partial(crps_kernel, lat, ens, degrees, variables),
        name="crps",
        compiler_params=PARAMS,
        in_specs=[scalar, whole, whole, whole],
        out_specs=whole,
        out_shape=sent,
        scratch_shapes=[
            VMEM((local, ens // 2, WIDTH, LANES), F32),
            VMEM((MEMBERS * VROWS, all_lines), F32),
            VMEM((MEMBERS * VROWS, padded), F32),
            VMEM((MEMBERS * VROWS, padded), BF16),
            VMEM((local, ens // 2, WIDTH, LANES), F32),
        ],
    )(own_wave, recv, observed, basis)
    recv = exchange(send)

    sensitivity, scores = pl.pallas_call(
        functools.partial(grid_kernel, lat, ens, variables),
        name="grid",
        compiler_params=PARAMS,
        in_specs=[scalar, whole, whole],
        out_specs=[far, whole],
        out_shape=[
            jax.ShapeDtypeStruct((local, span, nodes), BF16),
            jax.ShapeDtypeStruct((2, 2, variables), F32),
        ],
        scratch_shapes=[
            VMEM((local, span, nodes), BF16),
            pltpu.SemaphoreType.DMA((6,)),
        ],
    )(at_lat.reshape(1), recv, table)
    return sensitivity.reshape(predicted_grid.shape), scores.transpose(2, 0, 1)


def solution(mesh):
    placed = (P("ens", None, "lat", None), P(None, None, "lat", None), P("lat", None, None), P())
    return jax.shard_map(
        body,
        mesh=mesh,
        in_specs=placed,
        out_specs=(P("ens", None, "lat", None), P(None, None, "lat")),
        check_vma=False,
    )
```

```python
import functools
import math

import jax
import jax.numpy as jnp
from jax import lax
from jax.experimental import pallas as pl
from jax.experimental.pallas import tpu as pltpu
from jax.sharding import Mesh, PartitionSpec as P

SMOOTH = 0.1
LANES = 128
VROWS = 40
WIDTH = 640
MEMBERS = 8
F32 = jnp.float32
BF16 = jnp.bfloat16
VMEM = pltpu.VMEM
PARAMS = pltpu.CompilerParams(vmem_limit_bytes=16 * 1024 * 1024)
GROUP = ("ens", "chip")


def dot(a, b, dims):
    return lax.dot_general(a, b, (dims, ((), ())), preferred_element_type=F32)


def fourier_kernel(chips, core_ref, z_far, x_ref, send_ref, table_far, z_ref, x_vmem, table_ref, sems):
    width, nodes = x_vmem.shape
    rows = x_ref.shape[0]
    waves = pltpu.make_async_copy(z_far, z_ref, sems.at[0])
    waves.start()
    half = rows // 2
    copies = [
        pltpu.make_async_copy(x_ref.at[pl.ds(a, half)], x_vmem.at[pl.ds(a, half)], sems.at[1 + a // half])
        for a in range(0, rows, half)
    ]
    for copy in copies:
        copy.start()
    x_vmem[rows:, :] = jnp.zeros((width - rows, nodes), BF16)
    count = table_ref.shape[0]
    group = count // 2
    core = core_ref[0]
    shape = (count, z_ref.shape[1])
    d = lax.broadcasted_iota(jnp.int32, shape, 0)
    s = lax.broadcasted_iota(jnp.int32, shape, 1)
    other = lax.div(d, group)
    their_core = core + other - 2 * core * other
    slot = lax.div(lax.rem(d, group), 2 * chips)
    wanted = 2 * (2 * lax.rem(d, chips) + their_core) + slot
    waves.wait()
    z = jnp.sum(jnp.where(s == wanted, z_ref[...].astype(F32), 0.0), axis=1, keepdims=True)
    step = 2.0 * math.pi / nodes

    def cosine(p):
        p = p - nodes * jnp.floor(p * (1.0 / nodes))
        w = (jnp.abs(p - nodes / 2) - nodes / 4) * step
        w2 = w * w
        poly = -2.5052108e-08
        for c in (2.7557319e-06, -1.9841270e-04, 8.3333333e-03, -1.6666667e-01):
            poly = poly * w2 + c
        return w + w * (w2 * poly)

    j = lax.broadcasted_iota(jnp.int32, (1, LANES), 1).astype(F32)
    turn = nodes // 4
    for base in range(0, count, 2 * chips):
        for at in range(base, base + chips, 16):
            wave = jnp.broadcast_to(z[at : at + 16], (16, LANES))
            phase = wave * j
            real, imag = cosine(phase), cosine(phase + turn)
            ahead = wave * LANES
            keep_part, swap_part = cosine(ahead), cosine(ahead + turn)
            for b in range(0, nodes, LANES):
                n = min(LANES, nodes - b)
                table_ref[at : at + 16, b : b + n] = real[:, :n].astype(BF16)
                table_ref[at + chips : at + chips + 16, b : b + n] = imag[:, :n].astype(BF16)
                real, imag = (
                    real * keep_part - imag * swap_part,
                    imag * keep_part + real * swap_part,
                )
    keep = pltpu.make_async_copy(table_ref, table_far, sems.at[3])
    keep.start()
    for copy in copies:
        copy.wait()
    spectra = dot(table_ref[...], x_vmem[...], ((1,), (1,))) * nodes**-0.5
    for q in range(2):
        send_ref[:, q, :] = spectra[q * group : (q + 1) * group].astype(BF16)
    keep.wait()


def basis_kernel(chips, where_ref, p_ref, v_ref, basis_ref, obs_ref, p_vmem, v_vmem, mine, sems):
    slot = where_ref[0]
    core = where_ref[2]
    first = pltpu.make_async_copy(p_ref, p_vmem, sems.at[0])
    second = pltpu.make_async_copy(v_ref.at[:, where_ref[1]], v_vmem, sems.at[1])
    first.start()
    second.start()
    degrees, _, lines = p_vmem.shape
    first.wait()
    step = 16

    def pick(start, size):
        both = p_vmem[pl.ds(start, size)].astype(F32)
        chosen = jnp.where(slot == 0, both[:, 0, :], both[:, 1, :])
        mine[pl.ds(start, size), :] = chosen.astype(BF16)

    def one(i, carry):
        pick(pl.multiple_of(i * step, step), step)
        return carry

    lax.fori_loop(0, degrees // step, one, 0)
    rest = degrees % step
    if rest:
        pick(degrees - rest, rest)
    rows = lines // (2 * chips)
    source = lax.broadcasted_iota(jnp.int32, (lines, lines), 0)
    target = lax.broadcasted_iota(jnp.int32, (lines, lines), 1)
    other = lax.rem(lax.div(target, chips), 2)
    their_core = core + other - 2 * core * other
    line = rows * (2 * lax.rem(target, chips) + their_core) + lax.div(target, 2 * chips)
    order = source == line
    turned = dot(mine[...], order.astype(F32).astype(BF16), ((1,), (0,)))
    basis_ref[...] = turned.astype(BF16)
    second.wait()
    seen = v_vmem[...]
    obs_ref[...] = jnp.zeros(obs_ref.shape, F32)
    obs_ref[: seen.shape[0], :degrees] = jnp.where(slot == 0, seen[:, 0, :], seen[:, 1, :])


def swap_groups(parts, chips):
    lane = lax.broadcasted_iota(jnp.int32, parts[0].shape, 1)
    for distance in (2, 1):
        low = lax.rem(lax.div(lane, chips * distance), 2) == 0
        shift = chips * distance
        out = [None] * 4
        for j in range(4):
            if j & distance:
                continue
            a, b = parts[j], parts[j + distance]
            out[j] = jnp.where(low, a, pltpu.roll(b, shift, 1))
            out[j + distance] = jnp.where(low, pltpu.roll(a, LANES - shift, 1), b)
        parts = out
    return parts


def crps_kernel(
    chips, ens, degrees, variables,
    z_ref, own_ref, partner_ref, obs_ref, basis_ref, send_ref,
    turned, spectra, coeffs, grads, back,
):
    local = MEMBERS // ens
    span = variables * 8
    for q, ref in enumerate((own_ref, partner_ref)):
        turned[q] = ref[:, q, :].astype(F32).T
    for t2 in range(4):
        for m in range(local):
            parts = [
                turned[j % 2, pl.ds(m * span + 2 * t2 + j // 2, VROWS, stride=8), :] for j in range(4)
            ]
            for k, part in enumerate(swap_groups(parts, chips)):
                e = k * local + m
                spectra[pl.ds(e * VROWS, VROWS), pl.ds(t2 * LANES, LANES)] = part
    coeffs[:, :degrees] = dot(spectra[...].astype(BF16), basis_ref[...], ((1,), (1,)))

    zonal = z_ref[0]
    factor = jnp.where(zonal == 0, 1.0, 2.0).astype(F32)
    tiles = VROWS // 8

    def one_block(b, totals):
        lanes = pl.ds(pl.multiple_of(b * LANES, LANES), LANES)
        degree = b * LANES + lax.broadcasted_iota(jnp.int32, (8, LANES), 1)
        active = (degree >= zonal) & (degree < degrees)
        sums = []
        for tile in range(tiles):
            c = [coeffs[pl.ds(e * VROWS + tile * 8, 8), lanes] for e in range(MEMBERS)]
            seen = obs_ref[pl.ds(tile * 8, 8), lanes]
            slope = [None] * MEMBERS
            spread = None
            for e in range(MEMBERS - 1):
                part = None
                for f in range(e + 1, MEMBERS):
                    gap = c[e] - c[f]
                    square = gap * gap + SMOOTH * SMOOTH
                    inverse = lax.rsqrt(square)
                    sign = gap * inverse
                    root = square * inverse
                    part = root if part is None else part + root
                    slope[e] = sign if slope[e] is None else slope[e] + sign
                    slope[f] = -sign if slope[f] is None else slope[f] - sign
                part = part - SMOOTH * (MEMBERS - 1 - e)
                spread = part if spread is None else spread + part
            miss = None
            for e in range(MEMBERS):
                gap = c[e] - seen
                square = gap * gap + SMOOTH * SMOOTH
                inverse = lax.rsqrt(square)
                root = square * inverse
                miss = root if miss is None else miss + root
                grad = factor * (gap * inverse * (1 / MEMBERS) - slope[e] * (1 / MEMBERS**2))
                grad = jnp.where(active, grad, 0.0)
                grads[pl.ds(e * VROWS + tile * 8, 8), lanes] = grad.astype(BF16)
            miss = miss - SMOOTH * MEMBERS
            score = miss * (1 / MEMBERS) - spread * (1 / MEMBERS**2)
            sums.append(totals[tile] + jnp.where(active, factor * score, 0.0))
        return tuple(sums)

    blocks = coeffs.shape[1] // LANES
    zero = jnp.zeros((8, LANES), F32)
    totals = lax.fori_loop(0, blocks, one_block, (zero,) * tiles)

    returned = dot(grads[:, :degrees], basis_ref[...], ((1,), (0,)))
    for m in range(local):
        for t2 in range(4):
            parts = []
            for k in range(ens):
                e = k * local + m
                parts.append(returned[e * VROWS : (e + 1) * VROWS, t2 * LANES : (t2 + 1) * LANES])
            for j, part in enumerate(swap_groups(parts, chips)):
                back[j % 2, pl.ds(m * span + 2 * t2 + j // 2, VROWS, stride=8), :] = part
    base = local * span
    for tile in range(tiles):
        rest = jnp.sum(totals[tile], axis=1, keepdims=True) * (1.0 / degrees)
        for q in range(2):
            piece = rest.astype(BF16).astype(F32)
            rest = rest - piece
            back[q, pl.ds(base + tile * 8, 8), :] = jnp.broadcast_to(piece, (8, LANES))
    for q in range(2):
        back[q, base + VROWS :, :] = jnp.zeros((WIDTH - base - VROWS, LANES), F32)
        send_ref[:, q, :] = back[q].T.astype(BF16)


def grid_kernel(chips, ens, variables, at_ref, own_ref, partner_ref, table_ref, out_ref, score_ref, block, sems):
    rows, nodes = out_ref.shape
    scale = nodes**-0.5
    turned = jnp.concatenate(
        [ref[:, q, :].astype(F32).T.astype(BF16) for q, ref in enumerate((own_ref, partner_ref))], axis=1
    )
    copies = []
    for a in range(0, rows, LANES):
        n = min(LANES, rows - a)
        part = dot(turned[a : a + n, :], table_ref[...], ((1,), (0,))) * scale
        block[a : a + n, :] = part.astype(BF16)
        copy = pltpu.make_async_copy(block.at[pl.ds(a, n)], out_ref.at[pl.ds(a, n)], sems.at[len(copies)])
        copy.start()
        copies.append(copy)
    base = WIDTH - LANES
    mine = lax.broadcasted_iota(jnp.int32, (chips, LANES), 0) == at_ref[0]
    for k in range(ens):
        total = None
        for q in range(2):
            term = own_ref[k * chips : (k + 1) * chips, q, base:].astype(F32)
            term = jnp.sum(jnp.where(mine, term, 0.0), axis=0, keepdims=True)
            total = term if total is None else total + term
        total = pltpu.roll(total, LANES - (rows - base), 1)
        score_ref[k % 2, k // 2 : k // 2 + 1, :] = total[:, :variables]
    for copy in copies:
        copy.wait()


def far_of(*arrays):
    return [pltpu.with_memory_space_constraint(a, pltpu.HBM) for a in arrays]


def to_chips(values):
    return lax.all_to_all(values, GROUP, 0, 0, tiled=True)


def from_partner(values):
    return lax.ppermute(values, "core", [(0, 1), (1, 0)])


def body(predicted_grid, verifying_coefficients, weighted_polynomial_values, zonal_order_values):
    local, variables, lines, nodes = predicted_grid.shape
    slots, all_lines, degrees = weighted_polynomial_values.shape
    chips = lax.axis_size("chip")
    ens = lax.axis_size("ens")
    group = chips * ens
    count = 2 * group
    rows = local * variables * lines
    padded = -(-degrees // LANES) * LANES
    whole = pl.BlockSpec(memory_space=VMEM)
    scalar = pl.BlockSpec(memory_space=pltpu.SMEM)
    far = pl.BlockSpec(memory_space=pltpu.HBM)
    chip = lax.axis_index("chip")
    core = lax.axis_index("core")
    at_ens = lax.axis_index("ens")
    slot = at_ens // 2
    sent = jax.ShapeDtypeStruct((group, 2, WIDTH), BF16)

    send, table = pl.pallas_call(
        functools.partial(fourier_kernel, chips),
        name="fourier",
        compiler_params=PARAMS,
        in_specs=[scalar, far, far],
        out_specs=[whole, far],
        out_shape=[sent, pltpu.HBM((count, nodes), BF16)],
        scratch_shapes=[
            VMEM((1, zonal_order_values.shape[0]), jnp.int32),
            VMEM((WIDTH, nodes), BF16),
            VMEM((count, nodes), BF16),
            pltpu.SemaphoreType.DMA((4,)),
        ],
    )(core.reshape(1), *far_of(zonal_order_values.reshape(1, -1), predicted_grid.reshape(rows, nodes)))
    own = to_chips(send)

    basis, observed = pl.pallas_call(
        functools.partial(basis_kernel, chips),
        name="basis",
        compiler_params=PARAMS,
        in_specs=[scalar, far, far],
        out_specs=[whole, whole],
        out_shape=[
            jax.ShapeDtypeStruct((degrees, all_lines), BF16),
            jax.ShapeDtypeStruct((VROWS, padded), F32),
        ],
        scratch_shapes=[
            VMEM((degrees, slots, all_lines), BF16),
            VMEM((variables, slots, degrees), F32),
            VMEM((degrees, all_lines), BF16),
            pltpu.SemaphoreType.DMA((2,)),
        ],
        cost_estimate=pl.CostEstimate(flops=2 * degrees * all_lines**2, bytes_accessed=4_000_000, transcendentals=0),
    )(
        jnp.stack([slot, at_ens % 2, core]),
        *far_of(weighted_polynomial_values.transpose(2, 0, 1), verifying_coefficients),
    )
    own, basis, observed = lax.optimization_barrier((own, basis, observed))
    partner = from_partner(own)
    own_wave = lax.dynamic_slice_in_dim(zonal_order_values, 2 * (2 * chip + core) + slot, 1)

    send = pl.pallas_call(
        functools.partial(crps_kernel, chips, ens, degrees, variables),
        name="crps",
        compiler_params=PARAMS,
        in_specs=[scalar, whole, whole, whole, whole],
        out_specs=whole,
        out_shape=sent,
        scratch_shapes=[
            VMEM((2, WIDTH, LANES), F32),
            VMEM((MEMBERS * VROWS, all_lines), F32),
            VMEM((MEMBERS * VROWS, padded), F32),
            VMEM((MEMBERS * VROWS, padded), BF16),
            VMEM((2, WIDTH, LANES), F32),
        ],
    )(own_wave, own, partner, observed, basis)
    own = to_chips(send)
    partner = from_partner(own)

    sensitivity, scores = pl.pallas_call(
        functools.partial(grid_kernel, chips, ens, variables),
        name="grid",
        compiler_params=PARAMS,
        in_specs=[scalar, whole, whole, whole],
        out_specs=[far, whole],
        out_shape=[
            jax.ShapeDtypeStruct((rows, nodes), BF16),
            jax.ShapeDtypeStruct((2, 2, variables), F32),
        ],
        scratch_shapes=[VMEM((rows, nodes), BF16), pltpu.SemaphoreType.DMA((5,))],
    )(chip.reshape(1), own, partner, table)
    return sensitivity.reshape(predicted_grid.shape), scores.transpose(2, 0, 1)


def solution(mesh):
    lat, ens = mesh.devices.shape
    fine = Mesh(mesh.devices.reshape(lat // 2, 2, ens), ("chip", "core", "ens"))
    block = ("chip", "core")
    placed = (P("ens", None, block, None), P(None, None, block, None), P(block, None, None), P())
    return jax.shard_map(
        body,
        mesh=fine,
        in_specs=placed,
        out_specs=(P("ens", None, block, None), P(None, None, block)),
        check_vma=False,
    )
```

```python
import functools
import math

import jax
import jax.numpy as jnp
from jax import lax
from jax.experimental import pallas as pl
from jax.experimental.pallas import tpu as pltpu
from jax.sharding import Mesh, PartitionSpec as P

SMOOTH = 0.1
LANES = 128
VROWS = 40
WIDTH = 640
MEMBERS = 8
F32 = jnp.float32
BF16 = jnp.bfloat16
VMEM = pltpu.VMEM
PARAMS = pltpu.CompilerParams(vmem_limit_bytes=16 * 1024 * 1024)
GROUP = ("ens", "chip")


def dot(a, b, dims):
    return lax.dot_general(a, b, (dims, ((), ())), preferred_element_type=F32)


def fourier_kernel(chips, core_ref, z_far, x_ref, send_ref, table_far, z_ref, x_vmem, table_ref, sems):
    width, nodes = x_vmem.shape
    rows = x_ref.shape[0]
    waves = pltpu.make_async_copy(z_far, z_ref, sems.at[0])
    waves.start()
    half = rows // 2
    copies = [
        pltpu.make_async_copy(x_ref.at[pl.ds(a, half)], x_vmem.at[pl.ds(a, half)], sems.at[1 + a // half])
        for a in range(0, rows, half)
    ]
    for copy in copies:
        copy.start()
    x_vmem[rows:, :] = jnp.zeros((width - rows, nodes), BF16)
    count = table_ref.shape[0]
    group = count // 2
    core = core_ref[0]
    shape = (count, z_ref.shape[1])
    d = lax.broadcasted_iota(jnp.int32, shape, 0)
    s = lax.broadcasted_iota(jnp.int32, shape, 1)
    other = lax.div(d, group)
    their_core = core + other - 2 * core * other
    slot = lax.div(lax.rem(d, group), 2 * chips)
    wanted = 2 * (2 * lax.rem(d, chips) + their_core) + slot
    waves.wait()
    z = jnp.sum(jnp.where(s == wanted, z_ref[...].astype(F32), 0.0), axis=1, keepdims=True)
    step = 2.0 * math.pi / nodes

    def cosine(p):
        p = p - nodes * jnp.floor(p * (1.0 / nodes))
        w = (jnp.abs(p - nodes / 2) - nodes / 4) * step
        w2 = w * w
        poly = -2.5052108e-08
        for c in (2.7557319e-06, -1.9841270e-04, 8.3333333e-03, -1.6666667e-01):
            poly = poly * w2 + c
        return w + w * (w2 * poly)

    j = lax.broadcasted_iota(jnp.int32, (1, LANES), 1).astype(F32)
    turn = nodes // 4
    for base in range(0, count, 2 * chips):
        for at in range(base, base + chips, 16):
            wave = jnp.broadcast_to(z[at : at + 16], (16, LANES))
            phase = wave * j
            real, imag = cosine(phase), cosine(phase + turn)
            ahead = wave * LANES
            keep_part, swap_part = cosine(ahead), cosine(ahead + turn)
            for b in range(0, nodes, LANES):
                n = min(LANES, nodes - b)
                table_ref[at : at + 16, b : b + n] = real[:, :n].astype(BF16)
                table_ref[at + chips : at + chips + 16, b : b + n] = imag[:, :n].astype(BF16)
                real, imag = (
                    real * keep_part - imag * swap_part,
                    imag * keep_part + real * swap_part,
                )
    keep = pltpu.make_async_copy(table_ref, table_far, sems.at[3])
    keep.start()
    for copy in copies:
        copy.wait()
    spectra = dot(table_ref[...], x_vmem[...], ((1,), (1,))) * nodes**-0.5
    for q in range(2):
        send_ref[:, q, :] = spectra[q * group : (q + 1) * group].astype(BF16)
    keep.wait()


def basis_kernel(chips, where_ref, p_ref, v_ref, basis_ref, obs_ref, p_vmem, v_vmem, mine, sems):
    slot = where_ref[0]
    core = where_ref[2]
    first = pltpu.make_async_copy(p_ref, p_vmem, sems.at[0])
    second = pltpu.make_async_copy(v_ref.at[:, where_ref[1]], v_vmem, sems.at[1])
    first.start()
    second.start()
    degrees, _, lines = p_vmem.shape
    first.wait()
    step = 16

    def pick(start, size):
        both = p_vmem[pl.ds(start, size)].astype(F32)
        chosen = jnp.where(slot == 0, both[:, 0, :], both[:, 1, :])
        mine[pl.ds(start, size), :] = chosen.astype(BF16)

    def one(i, carry):
        pick(pl.multiple_of(i * step, step), step)
        return carry

    lax.fori_loop(0, degrees // step, one, 0)
    rest = degrees % step
    if rest:
        pick(degrees - rest, rest)
    rows = lines // (2 * chips)
    source = lax.broadcasted_iota(jnp.int32, (lines, lines), 0)
    target = lax.broadcasted_iota(jnp.int32, (lines, lines), 1)
    other = lax.div(target, lines // 2)
    their_core = core + other - 2 * core * other
    row = lax.div(lax.rem(target, lines // 2), chips)
    line = rows * (2 * lax.rem(target, chips) + their_core) + row
    order = source == line
    turned = dot(mine[...], order.astype(F32).astype(BF16), ((1,), (0,)))
    basis_ref[...] = turned.astype(BF16)
    second.wait()
    seen = v_vmem[...]
    obs_ref[...] = jnp.zeros(obs_ref.shape, F32)
    obs_ref[: seen.shape[0], :degrees] = jnp.where(slot == 0, seen[:, 0, :], seen[:, 1, :])


def swap_groups(parts, chips):
    lane = lax.broadcasted_iota(jnp.int32, parts[0].shape, 1)
    for distance in (2, 1):
        low = lax.rem(lax.div(lane, chips * distance), 2) == 0
        shift = chips * distance
        out = [None] * 4
        for j in range(4):
            if j & distance:
                continue
            a, b = parts[j], parts[j + distance]
            out[j] = jnp.where(low, a, pltpu.roll(b, shift, 1))
            out[j + distance] = jnp.where(low, pltpu.roll(a, LANES - shift, 1), b)
        parts = out
    return parts


def turn_lines(ref, q, turned, spectra, chips, ens, variables):
    local = MEMBERS // ens
    span = variables * 8
    turned[...] = ref[:, q, :].astype(F32).T
    for h in range(2):
        for m in range(local):
            parts = [turned[pl.ds(m * span + 4 * h + j, VROWS, stride=8), :] for j in range(4)]
            for k, part in enumerate(swap_groups(parts, chips)):
                e = k * local + m
                spectra[pl.ds(e * VROWS, VROWS), pl.ds(h * LANES, LANES)] = part
    return spectra[...].astype(BF16)


def own_kernel(chips, ens, variables, own_ref, basis_ref, coeffs_ref, turned, spectra):
    degrees, lines = basis_ref.shape
    members = turn_lines(own_ref, 0, turned, spectra, chips, ens, variables)
    coeffs_ref[:, :degrees] = dot(members, basis_ref[:, : lines // 2], ((1,), (1,)))


def crps_kernel(
    chips, ens, degrees, variables,
    z_ref, partner_ref, own_coeffs_ref, obs_ref, basis_ref, send_ref,
    turned, spectra, coeffs, grads, back,
):
    local = MEMBERS // ens
    span = variables * 8
    half = basis_ref.shape[1] // 2
    members = turn_lines(partner_ref, 1, turned, spectra, chips, ens, variables)
    coeffs[:, :degrees] = own_coeffs_ref[:, :degrees] + dot(members, basis_ref[:, half:], ((1,), (1,)))

    zonal = z_ref[0]
    factor = jnp.where(zonal == 0, 1.0, 2.0).astype(F32)
    tiles = VROWS // 8

    def one_block(b, totals):
        lanes = pl.ds(pl.multiple_of(b * LANES, LANES), LANES)
        degree = b * LANES + lax.broadcasted_iota(jnp.int32, (8, LANES), 1)
        active = (degree >= zonal) & (degree < degrees)
        sums = []
        for tile in range(tiles):
            c = [coeffs[pl.ds(e * VROWS + tile * 8, 8), lanes] for e in range(MEMBERS)]
            seen = obs_ref[pl.ds(tile * 8, 8), lanes]
            slope = [None] * MEMBERS
            spread = None
            for e in range(MEMBERS - 1):
                part = None
                for f in range(e + 1, MEMBERS):
                    gap = c[e] - c[f]
                    square = gap * gap + SMOOTH * SMOOTH
                    inverse = lax.rsqrt(square)
                    sign = gap * inverse
                    root = square * inverse
                    part = root if part is None else part + root
                    slope[e] = sign if slope[e] is None else slope[e] + sign
                    slope[f] = -sign if slope[f] is None else slope[f] - sign
                part = part - SMOOTH * (MEMBERS - 1 - e)
                spread = part if spread is None else spread + part
            miss = None
            for e in range(MEMBERS):
                gap = c[e] - seen
                square = gap * gap + SMOOTH * SMOOTH
                inverse = lax.rsqrt(square)
                root = square * inverse
                miss = root if miss is None else miss + root
                grad = factor * (gap * inverse * (1 / MEMBERS) - slope[e] * (1 / MEMBERS**2))
                grad = jnp.where(active, grad, 0.0)
                grads[pl.ds(e * VROWS + tile * 8, 8), lanes] = grad.astype(BF16)
            miss = miss - SMOOTH * MEMBERS
            score = miss * (1 / MEMBERS) - spread * (1 / MEMBERS**2)
            sums.append(totals[tile] + jnp.where(active, factor * score, 0.0))
        return tuple(sums)

    blocks = coeffs.shape[1] // LANES
    zero = jnp.zeros((8, LANES), F32)
    totals = lax.fori_loop(0, blocks, one_block, (zero,) * tiles)

    returned = dot(grads[:, :degrees], basis_ref[...], ((1,), (0,)))
    for m in range(local):
        for q in range(2):
            for h in range(2):
                at = (2 * q + h) * LANES
                parts = []
                for k in range(ens):
                    e = k * local + m
                    parts.append(returned[e * VROWS : (e + 1) * VROWS, at : at + LANES])
                for j, part in enumerate(swap_groups(parts, chips)):
                    back[q, pl.ds(m * span + 4 * h + j, VROWS, stride=8), :] = part
    base = local * span
    for tile in range(tiles):
        rest = jnp.sum(totals[tile], axis=1, keepdims=True) * (1.0 / degrees)
        for q in range(2):
            piece = rest.astype(BF16).astype(F32)
            rest = rest - piece
            back[q, pl.ds(base + tile * 8, 8), :] = jnp.broadcast_to(piece, (8, LANES))
    for q in range(2):
        back[q, base + VROWS :, :] = jnp.zeros((WIDTH - base - VROWS, LANES), F32)
        send_ref[:, q, :] = back[q].T.astype(BF16)


def score_kernel(chips, ens, variables, rows, at_ref, own_ref, turned_ref, score_ref):
    turned_ref[...] = own_ref[:, 0, :].astype(F32).T.astype(BF16)
    base = WIDTH - LANES
    mine = lax.broadcasted_iota(jnp.int32, (chips, LANES), 0) == at_ref[0]
    for k in range(ens):
        total = None
        for q in range(2):
            term = own_ref[k * chips : (k + 1) * chips, q, base:].astype(F32)
            term = jnp.sum(jnp.where(mine, term, 0.0), axis=0, keepdims=True)
            total = term if total is None else total + term
        total = pltpu.roll(total, LANES - (rows - base), 1)
        score_ref[k % 2, k // 2 : k // 2 + 1, :] = total[:, :variables]


def grid_kernel(partner_ref, own_ref, table_ref, out_ref, block, sems):
    rows, nodes = out_ref.shape
    scale = nodes**-0.5
    partner = partner_ref[:, 1, :].astype(F32).T.astype(BF16)
    turned = jnp.concatenate([own_ref[...], partner], axis=1)
    copies = []
    for a in range(0, rows, LANES):
        n = min(LANES, rows - a)
        part = dot(turned[a : a + n, :], table_ref[...], ((1,), (0,))) * scale
        block[a : a + n, :] = part.astype(BF16)
        copy = pltpu.make_async_copy(block.at[pl.ds(a, n)], out_ref.at[pl.ds(a, n)], sems.at[len(copies)])
        copy.start()
        copies.append(copy)
    for copy in copies:
        copy.wait()


def far_of(*arrays):
    return [pltpu.with_memory_space_constraint(a, pltpu.HBM) for a in arrays]


def to_chips(values):
    return lax.all_to_all(values, GROUP, 0, 0, tiled=True)


def from_partner(values):
    return lax.ppermute(values, "core", [(0, 1), (1, 0)])


def body(predicted_grid, verifying_coefficients, weighted_polynomial_values, zonal_order_values):
    local, variables, lines, nodes = predicted_grid.shape
    slots, all_lines, degrees = weighted_polynomial_values.shape
    chips = lax.axis_size("chip")
    ens = lax.axis_size("ens")
    group = chips * ens
    count = 2 * group
    rows = local * variables * lines
    padded = -(-degrees // LANES) * LANES
    whole = pl.BlockSpec(memory_space=VMEM)
    scalar = pl.BlockSpec(memory_space=pltpu.SMEM)
    far = pl.BlockSpec(memory_space=pltpu.HBM)
    chip = lax.axis_index("chip")
    core = lax.axis_index("core")
    at_ens = lax.axis_index("ens")
    slot = at_ens // 2
    sent = jax.ShapeDtypeStruct((group, 2, WIDTH), BF16)

    send, table = pl.pallas_call(
        functools.partial(fourier_kernel, chips),
        name="fourier",
        compiler_params=PARAMS,
        in_specs=[scalar, far, far],
        out_specs=[whole, far],
        out_shape=[sent, pltpu.HBM((count, nodes), BF16)],
        scratch_shapes=[
            VMEM((1, zonal_order_values.shape[0]), jnp.int32),
            VMEM((WIDTH, nodes), BF16),
            VMEM((count, nodes), BF16),
            pltpu.SemaphoreType.DMA((4,)),
        ],
    )(core.reshape(1), *far_of(zonal_order_values.reshape(1, -1), predicted_grid.reshape(rows, nodes)))
    own = to_chips(send)

    basis, observed = pl.pallas_call(
        functools.partial(basis_kernel, chips),
        name="basis",
        compiler_params=PARAMS,
        in_specs=[scalar, far, far],
        out_specs=[whole, whole],
        out_shape=[
            jax.ShapeDtypeStruct((degrees, all_lines), BF16),
            jax.ShapeDtypeStruct((VROWS, padded), F32),
        ],
        scratch_shapes=[
            VMEM((degrees, slots, all_lines), BF16),
            VMEM((variables, slots, degrees), F32),
            VMEM((degrees, all_lines), BF16),
            pltpu.SemaphoreType.DMA((2,)),
        ],
        cost_estimate=pl.CostEstimate(flops=2 * degrees * all_lines**2, bytes_accessed=4_000_000, transcendentals=0),
    )(
        jnp.stack([slot, at_ens % 2, core]),
        *far_of(weighted_polynomial_values.transpose(2, 0, 1), verifying_coefficients),
    )
    own, basis, observed = lax.optimization_barrier((own, basis, observed))
    partner = from_partner(own)
    own_wave = lax.dynamic_slice_in_dim(zonal_order_values, 2 * (2 * chip + core) + slot, 1)

    own_coeffs = pl.pallas_call(
        functools.partial(own_kernel, chips, ens, variables),
        name="own",
        compiler_params=PARAMS,
        in_specs=[whole, whole],
        out_specs=whole,
        out_shape=jax.ShapeDtypeStruct((MEMBERS * VROWS, padded), F32),
        scratch_shapes=[VMEM((WIDTH, LANES), F32), VMEM((MEMBERS * VROWS, all_lines // 2), F32)],
        cost_estimate=pl.CostEstimate(
            flops=MEMBERS * VROWS * all_lines * degrees, bytes_accessed=2_000_000, transcendentals=0
        ),
    )(own, basis)
    send = pl.pallas_call(
        functools.partial(crps_kernel, chips, ens, degrees, variables),
        name="crps",
        compiler_params=PARAMS,
        in_specs=[scalar, whole, whole, whole, whole],
        out_specs=whole,
        out_shape=sent,
        scratch_shapes=[
            VMEM((WIDTH, LANES), F32),
            VMEM((MEMBERS * VROWS, all_lines // 2), F32),
            VMEM((MEMBERS * VROWS, padded), F32),
            VMEM((MEMBERS * VROWS, padded), BF16),
            VMEM((2, WIDTH, LANES), F32),
        ],
    )(own_wave, partner, own_coeffs, observed, basis)
    own = to_chips(send)
    partner = from_partner(own)

    turned, scores = pl.pallas_call(
        functools.partial(score_kernel, chips, ens, variables, rows),
        name="score",
        compiler_params=PARAMS,
        in_specs=[scalar, whole],
        out_specs=[whole, whole],
        out_shape=[
            jax.ShapeDtypeStruct((WIDTH, group), BF16),
            jax.ShapeDtypeStruct((2, 2, variables), F32),
        ],
        cost_estimate=pl.CostEstimate(flops=20_000_000, bytes_accessed=500_000, transcendentals=0),
    )(chip.reshape(1), own)
    sensitivity = pl.pallas_call(
        grid_kernel,
        name="grid",
        compiler_params=PARAMS,
        in_specs=[whole, whole, whole],
        out_specs=far,
        out_shape=jax.ShapeDtypeStruct((rows, nodes), BF16),
        scratch_shapes=[VMEM((rows, nodes), BF16), pltpu.SemaphoreType.DMA((5,))],
    )(partner, turned, table)
    return sensitivity.reshape(predicted_grid.shape), scores.transpose(2, 0, 1)


def solution(mesh):
    lat, ens = mesh.devices.shape
    fine = Mesh(mesh.devices.reshape(lat // 2, 2, ens), ("chip", "core", "ens"))
    block = ("chip", "core")
    placed = (P("ens", None, block, None), P(None, None, block, None), P(block, None, None), P())
    return jax.shard_map(
        body,
        mesh=fine,
        in_specs=placed,
        out_specs=(P("ens", None, block, None), P(None, None, block)),
        check_vma=False,
    )
```

```python
import functools
import math

import jax
import jax.numpy as jnp
from jax import lax
from jax.experimental import pallas as pl
from jax.experimental.pallas import tpu as pltpu
from jax.sharding import Mesh, PartitionSpec as P

SMOOTH = 0.1
LANES = 128
VROWS = 40
WIDTH = 640
MEMBERS = 8
F32 = jnp.float32
BF16 = jnp.bfloat16
VMEM = pltpu.VMEM
PARAMS = pltpu.CompilerParams(vmem_limit_bytes=16 * 1024 * 1024)
GROUP = ("ens", "chip")


def dot(a, b, dims):
    return lax.dot_general(a, b, (dims, ((), ())), preferred_element_type=F32)


def fourier_kernel(chips, core_ref, z_far, x_ref, send_ref, table_far, z_ref, x_vmem, table_ref, sems):
    width, nodes = x_vmem.shape
    rows = x_ref.shape[0]
    waves = pltpu.make_async_copy(z_far, z_ref, sems.at[0])
    waves.start()
    half = rows // 2
    copies = [
        pltpu.make_async_copy(x_ref.at[pl.ds(a, half)], x_vmem.at[pl.ds(a, half)], sems.at[1 + a // half])
        for a in range(0, rows, half)
    ]
    for copy in copies:
        copy.start()
    x_vmem[rows:, :] = jnp.zeros((width - rows, nodes), BF16)
    count = table_ref.shape[0]
    group = count // 2
    core = core_ref[0]
    shape = (count, z_ref.shape[1])
    d = lax.broadcasted_iota(jnp.int32, shape, 0)
    s = lax.broadcasted_iota(jnp.int32, shape, 1)
    other = lax.div(d, group)
    their_core = core + other - 2 * core * other
    slot = lax.div(lax.rem(d, group), 2 * chips)
    wanted = 2 * (2 * lax.rem(d, chips) + their_core) + slot
    waves.wait()
    z = jnp.sum(jnp.where(s == wanted, z_ref[...].astype(F32), 0.0), axis=1, keepdims=True)
    step = 2.0 * math.pi / nodes

    def cosine(p):
        p = p - nodes * jnp.floor(p * (1.0 / nodes))
        w = (jnp.abs(p - nodes / 2) - nodes / 4) * step
        w2 = w * w
        poly = -2.5052108e-08
        for c in (2.7557319e-06, -1.9841270e-04, 8.3333333e-03, -1.6666667e-01):
            poly = poly * w2 + c
        return w + w * (w2 * poly)

    j = lax.broadcasted_iota(jnp.int32, (1, LANES), 1).astype(F32)
    turn = nodes // 4
    for base in range(0, count, 2 * chips):
        for at in range(base, base + chips, 16):
            wave = jnp.broadcast_to(z[at : at + 16], (16, LANES))
            phase = wave * j
            real, imag = cosine(phase), cosine(phase + turn)
            ahead = wave * LANES
            keep_part, swap_part = cosine(ahead), cosine(ahead + turn)
            for b in range(0, nodes, LANES):
                n = min(LANES, nodes - b)
                table_ref[at : at + 16, b : b + n] = real[:, :n].astype(BF16)
                table_ref[at + chips : at + chips + 16, b : b + n] = imag[:, :n].astype(BF16)
                real, imag = (
                    real * keep_part - imag * swap_part,
                    imag * keep_part + real * swap_part,
                )
    keep = pltpu.make_async_copy(table_ref, table_far, sems.at[3])
    keep.start()
    for copy in copies:
        copy.wait()
    spectra = dot(table_ref[...], x_vmem[...], ((1,), (1,))) * nodes**-0.5
    for q in range(2):
        send_ref[:, q, :] = spectra[q * group : (q + 1) * group].astype(BF16)
    keep.wait()


def basis_kernel(chips, where_ref, p_ref, v_ref, basis_ref, obs_ref, p_vmem, v_vmem, mine, sems):
    slot = where_ref[0]
    core = where_ref[2]
    first = pltpu.make_async_copy(p_ref, p_vmem, sems.at[0])
    second = pltpu.make_async_copy(v_ref.at[:, where_ref[1]], v_vmem, sems.at[1])
    first.start()
    second.start()
    degrees, _, lines = p_vmem.shape
    first.wait()
    step = 16

    def pick(start, size):
        both = p_vmem[pl.ds(start, size)].astype(F32)
        chosen = jnp.where(slot == 0, both[:, 0, :], both[:, 1, :])
        mine[pl.ds(start, size), :] = chosen.astype(BF16)

    def one(i, carry):
        pick(pl.multiple_of(i * step, step), step)
        return carry

    lax.fori_loop(0, degrees // step, one, 0)
    rest = degrees % step
    if rest:
        pick(degrees - rest, rest)
    rows = lines // (2 * chips)
    source = lax.broadcasted_iota(jnp.int32, (lines, lines), 0)
    target = lax.broadcasted_iota(jnp.int32, (lines, lines), 1)
    other = lax.div(target, lines // 2)
    their_core = core + other - 2 * core * other
    row = lax.div(lax.rem(target, lines // 2), chips)
    line = rows * (2 * lax.rem(target, chips) + their_core) + row
    order = source == line
    turned = dot(mine[...], order.astype(F32).astype(BF16), ((1,), (0,)))
    basis_ref[:degrees, :] = turned.astype(BF16)
    basis_ref[degrees:, :] = jnp.zeros((basis_ref.shape[0] - degrees, lines), BF16)
    second.wait()
    seen = v_vmem[...]
    obs_ref[...] = jnp.zeros(obs_ref.shape, F32)
    obs_ref[: seen.shape[0], :degrees] = jnp.where(slot == 0, seen[:, 0, :], seen[:, 1, :])


def swap_groups(parts, chips):
    lane = lax.broadcasted_iota(jnp.int32, parts[0].shape, 1)
    for distance in (2, 1):
        low = lax.rem(lax.div(lane, chips * distance), 2) == 0
        shift = chips * distance
        out = [None] * 4
        for j in range(4):
            if j & distance:
                continue
            a, b = parts[j], parts[j + distance]
            out[j] = jnp.where(low, a, pltpu.roll(b, shift, 1))
            out[j + distance] = jnp.where(low, pltpu.roll(a, LANES - shift, 1), b)
        parts = out
    return parts


def turn_lines(ref, q, turned, spectra, chips, ens, variables):
    local = MEMBERS // ens
    span = variables * 8
    turned[...] = ref[:, q, :].astype(F32).T
    for h in range(2):
        for m in range(local):
            parts = [turned[pl.ds(m * span + 4 * h + j, VROWS, stride=8), :] for j in range(4)]
            for k, part in enumerate(swap_groups(parts, chips)):
                e = k * local + m
                spectra[pl.ds(e * VROWS, VROWS), pl.ds(h * LANES, LANES)] = part
    return spectra[...].astype(BF16)


def own_kernel(chips, ens, variables, own_ref, basis_ref, coeffs_ref, turned, spectra):
    lines = basis_ref.shape[1]
    members = turn_lines(own_ref, 0, turned, spectra, chips, ens, variables)
    coeffs_ref[...] = dot(members, basis_ref[:, : lines // 2], ((1,), (1,)))


def crps_kernel(
    chips, ens, degrees, variables,
    z_ref, partner_ref, own_coeffs_ref, obs_ref, basis_ref, send_ref,
    turned, spectra, coeffs, grads, back,
):
    local = MEMBERS // ens
    span = variables * 8
    half = basis_ref.shape[1] // 2
    members = turn_lines(partner_ref, 1, turned, spectra, chips, ens, variables)
    coeffs[...] = own_coeffs_ref[...] + dot(members, basis_ref[:, half:], ((1,), (1,)))

    zonal = z_ref[0]
    factor = jnp.where(zonal == 0, 1.0, 2.0).astype(F32)
    tiles = VROWS // 8

    def one_block(b, totals):
        lanes = pl.ds(pl.multiple_of(b * LANES, LANES), LANES)
        degree = b * LANES + lax.broadcasted_iota(jnp.int32, (8, LANES), 1)
        active = (degree >= zonal) & (degree < degrees)
        sums = []
        for tile in range(tiles):
            c = [coeffs[pl.ds(e * VROWS + tile * 8, 8), lanes] for e in range(MEMBERS)]
            seen = obs_ref[pl.ds(tile * 8, 8), lanes]
            slope = [None] * MEMBERS
            spread = None
            inverses = None
            for e in range(MEMBERS - 1):
                for f in range(e + 1, MEMBERS):
                    gap = c[e] - c[f]
                    inverse = lax.rsqrt(gap * gap + SMOOTH * SMOOTH)
                    sign = gap * inverse
                    inverses = inverse if inverses is None else inverses + inverse
                    slope[e] = sign if slope[e] is None else slope[e] + sign
                    slope[f] = -sign if slope[f] is None else slope[f] - sign
            for e in range(1, MEMBERS):
                part = (c[e] - c[0]) * slope[e]
                spread = part if spread is None else spread + part
            pairs = MEMBERS * (MEMBERS - 1) // 2
            spread = spread + (inverses * (SMOOTH * SMOOTH) - SMOOTH * pairs)
            miss = None
            for e in range(MEMBERS):
                gap = c[e] - seen
                square = gap * gap + SMOOTH * SMOOTH
                inverse = lax.rsqrt(square)
                root = square * inverse
                miss = root if miss is None else miss + root
                grad = factor * (gap * inverse * (1 / MEMBERS) - slope[e] * (1 / MEMBERS**2))
                grad = jnp.where(active, grad, 0.0)
                grads[pl.ds(e * VROWS + tile * 8, 8), lanes] = grad.astype(BF16)
            miss = miss - SMOOTH * MEMBERS
            score = miss * (1 / MEMBERS) - spread * (1 / MEMBERS**2)
            sums.append(totals[tile] + jnp.where(active, factor * score, 0.0))
        return tuple(sums)

    blocks = coeffs.shape[1] // LANES
    zero = jnp.zeros((8, LANES), F32)
    totals = lax.fori_loop(0, blocks, one_block, (zero,) * tiles, unroll=6)

    returned = dot(grads[...], basis_ref[...], ((1,), (0,)))
    for m in range(local):
        for q in range(2):
            for h in range(2):
                at = (2 * q + h) * LANES
                parts = []
                for k in range(ens):
                    e = k * local + m
                    parts.append(returned[e * VROWS : (e + 1) * VROWS, at : at + LANES])
                for j, part in enumerate(swap_groups(parts, chips)):
                    back[q, pl.ds(m * span + 4 * h + j, VROWS, stride=8), :] = part
    base = local * span
    for tile in range(tiles):
        rest = jnp.sum(totals[tile], axis=1, keepdims=True) * (1.0 / degrees)
        for q in range(2):
            piece = rest.astype(BF16).astype(F32)
            rest = rest - piece
            back[q, pl.ds(base + tile * 8, 8), :] = jnp.broadcast_to(piece, (8, LANES))
    for q in range(2):
        back[q, base + VROWS :, :] = jnp.zeros((WIDTH - base - VROWS, LANES), F32)
        send_ref[:, q, :] = back[q].T.astype(BF16)


def score_kernel(chips, ens, variables, rows, at_ref, own_ref, turned_ref, score_ref):
    turned_ref[...] = own_ref[:, 0, :].astype(F32).T.astype(BF16)
    base = WIDTH - LANES
    mine = lax.broadcasted_iota(jnp.int32, (chips, LANES), 0) == at_ref[0]
    for k in range(ens):
        total = None
        for q in range(2):
            term = own_ref[k * chips : (k + 1) * chips, q, base:].astype(F32)
            term = jnp.sum(jnp.where(mine, term, 0.0), axis=0, keepdims=True)
            total = term if total is None else total + term
        total = pltpu.roll(total, LANES - (rows - base), 1)
        score_ref[k % 2, k // 2 : k // 2 + 1, :] = total[:, :variables]


def grid_kernel(partner_ref, own_ref, table_ref, out_ref, block, sems):
    rows, nodes = out_ref.shape
    scale = nodes**-0.5
    partner = partner_ref[:, 1, :].astype(F32).T.astype(BF16)
    turned = jnp.concatenate([own_ref[...], partner], axis=1)
    copies = []
    for a in range(0, rows, LANES):
        n = min(LANES, rows - a)
        part = dot(turned[a : a + n, :], table_ref[...], ((1,), (0,))) * scale
        block[a : a + n, :] = part.astype(BF16)
        copy = pltpu.make_async_copy(block.at[pl.ds(a, n)], out_ref.at[pl.ds(a, n)], sems.at[len(copies)])
        copy.start()
        copies.append(copy)
    for copy in copies:
        copy.wait()


def far_of(*arrays):
    return [pltpu.with_memory_space_constraint(a, pltpu.HBM) for a in arrays]


def to_chips(values):
    return lax.all_to_all(values, GROUP, 0, 0, tiled=True)


def from_partner(values):
    return lax.ppermute(values, "core", [(0, 1), (1, 0)])


def body(predicted_grid, verifying_coefficients, weighted_polynomial_values, zonal_order_values):
    local, variables, lines, nodes = predicted_grid.shape
    slots, all_lines, degrees = weighted_polynomial_values.shape
    chips = lax.axis_size("chip")
    ens = lax.axis_size("ens")
    group = chips * ens
    count = 2 * group
    rows = local * variables * lines
    padded = -(-degrees // LANES) * LANES
    whole = pl.BlockSpec(memory_space=VMEM)
    scalar = pl.BlockSpec(memory_space=pltpu.SMEM)
    far = pl.BlockSpec(memory_space=pltpu.HBM)
    chip = lax.axis_index("chip")
    core = lax.axis_index("core")
    at_ens = lax.axis_index("ens")
    slot = at_ens // 2
    sent = jax.ShapeDtypeStruct((group, 2, WIDTH), BF16)

    send, table = pl.pallas_call(
        functools.partial(fourier_kernel, chips),
        name="fourier",
        compiler_params=PARAMS,
        in_specs=[scalar, far, far],
        out_specs=[whole, far],
        out_shape=[sent, pltpu.HBM((count, nodes), BF16)],
        scratch_shapes=[
            VMEM((1, zonal_order_values.shape[0]), jnp.int32),
            VMEM((WIDTH, nodes), BF16),
            VMEM((count, nodes), BF16),
            pltpu.SemaphoreType.DMA((4,)),
        ],
    )(core.reshape(1), *far_of(zonal_order_values.reshape(1, -1), predicted_grid.reshape(rows, nodes)))
    own = to_chips(send)

    basis, observed = pl.pallas_call(
        functools.partial(basis_kernel, chips),
        name="basis",
        compiler_params=PARAMS,
        in_specs=[scalar, far, far],
        out_specs=[whole, whole],
        out_shape=[
            jax.ShapeDtypeStruct((padded, all_lines), BF16),
            jax.ShapeDtypeStruct((VROWS, padded), F32),
        ],
        scratch_shapes=[
            VMEM((degrees, slots, all_lines), BF16),
            VMEM((variables, slots, degrees), F32),
            VMEM((degrees, all_lines), BF16),
            pltpu.SemaphoreType.DMA((2,)),
        ],
        cost_estimate=pl.CostEstimate(flops=2 * degrees * all_lines**2, bytes_accessed=4_000_000, transcendentals=0),
    )(
        jnp.stack([slot, at_ens % 2, core]),
        *far_of(weighted_polynomial_values.transpose(2, 0, 1), verifying_coefficients),
    )
    own, basis, observed = lax.optimization_barrier((own, basis, observed))
    partner = from_partner(own)
    own_wave = lax.dynamic_slice_in_dim(zonal_order_values, 2 * (2 * chip + core) + slot, 1)

    own_coeffs = pl.pallas_call(
        functools.partial(own_kernel, chips, ens, variables),
        name="own",
        compiler_params=PARAMS,
        in_specs=[whole, whole],
        out_specs=whole,
        out_shape=jax.ShapeDtypeStruct((MEMBERS * VROWS, padded), F32),
        scratch_shapes=[VMEM((WIDTH, LANES), F32), VMEM((MEMBERS * VROWS, all_lines // 2), F32)],
        cost_estimate=pl.CostEstimate(
            flops=MEMBERS * VROWS * all_lines * degrees, bytes_accessed=2_000_000, transcendentals=0
        ),
    )(own, basis)
    send = pl.pallas_call(
        functools.partial(crps_kernel, chips, ens, degrees, variables),
        name="crps",
        compiler_params=PARAMS,
        in_specs=[scalar, whole, whole, whole, whole],
        out_specs=whole,
        out_shape=sent,
        scratch_shapes=[
            VMEM((WIDTH, LANES), F32),
            VMEM((MEMBERS * VROWS, all_lines // 2), F32),
            VMEM((MEMBERS * VROWS, padded), F32),
            VMEM((MEMBERS * VROWS, padded), BF16),
            VMEM((2, WIDTH, LANES), F32),
        ],
    )(own_wave, partner, own_coeffs, observed, basis)
    own = to_chips(send)
    partner = from_partner(own)

    turned, scores = pl.pallas_call(
        functools.partial(score_kernel, chips, ens, variables, rows),
        name="score",
        compiler_params=PARAMS,
        in_specs=[scalar, whole],
        out_specs=[whole, whole],
        out_shape=[
            jax.ShapeDtypeStruct((WIDTH, group), BF16),
            jax.ShapeDtypeStruct((2, 2, variables), F32),
        ],
        cost_estimate=pl.CostEstimate(flops=20_000_000, bytes_accessed=500_000, transcendentals=0),
    )(chip.reshape(1), own)
    sensitivity = pl.pallas_call(
        grid_kernel,
        name="grid",
        compiler_params=PARAMS,
        in_specs=[whole, whole, whole],
        out_specs=far,
        out_shape=jax.ShapeDtypeStruct((rows, nodes), BF16),
        scratch_shapes=[VMEM((rows, nodes), BF16), pltpu.SemaphoreType.DMA((5,))],
    )(partner, turned, table)
    return sensitivity.reshape(predicted_grid.shape), scores.transpose(2, 0, 1)


def solution(mesh):
    lat, ens = mesh.devices.shape
    fine = Mesh(mesh.devices.reshape(lat // 2, 2, ens), ("chip", "core", "ens"))
    block = ("chip", "core")
    placed = (P("ens", None, block, None), P(None, None, block, None), P(block, None, None), P())
    return jax.shard_map(
        body,
        mesh=fine,
        in_specs=placed,
        out_specs=(P("ens", None, block, None), P(None, None, block)),
        check_vma=False,
    )
```

```python
import functools
import math

import jax
import jax.numpy as jnp
from jax import lax
from jax.experimental import pallas as pl
from jax.experimental.pallas import tpu as pltpu
from jax.sharding import Mesh, PartitionSpec as P

SMOOTH = 0.1
LANES = 128
VROWS = 40
WIDTH = 640
MEMBERS = 8
F32 = jnp.float32
BF16 = jnp.bfloat16
VMEM = pltpu.VMEM
PARAMS = pltpu.CompilerParams(vmem_limit_bytes=16 * 1024 * 1024)
GROUP = ("ens", "chip")


def dot(a, b, dims):
    return lax.dot_general(a, b, (dims, ((), ())), preferred_element_type=F32)


def fourier_kernel(chips, core_ref, z_far, x_ref, send_ref, table_far, z_ref, x_vmem, table_ref, sems):
    width, nodes = x_vmem.shape
    rows = x_ref.shape[0]
    waves = pltpu.make_async_copy(z_far, z_ref, sems.at[0])
    waves.start()
    half = rows // 2
    copies = [
        pltpu.make_async_copy(x_ref.at[pl.ds(a, half)], x_vmem.at[pl.ds(a, half)], sems.at[1 + a // half])
        for a in range(0, rows, half)
    ]
    for copy in copies:
        copy.start()
    x_vmem[rows:, :] = jnp.zeros((width - rows, nodes), BF16)
    count = table_ref.shape[0]
    group = count // 2
    core = core_ref[0]
    shape = (count, z_ref.shape[1])
    d = lax.broadcasted_iota(jnp.int32, shape, 0)
    s = lax.broadcasted_iota(jnp.int32, shape, 1)
    other = lax.div(d, group)
    their_core = core + other - 2 * core * other
    slot = lax.div(lax.rem(d, group), 2 * chips)
    wanted = 2 * (2 * lax.rem(d, chips) + their_core) + slot
    waves.wait()
    z = jnp.sum(jnp.where(s == wanted, z_ref[...].astype(F32), 0.0), axis=1, keepdims=True)
    step = 2.0 * math.pi / nodes

    def cosine(p):
        p = p - nodes * jnp.floor(p * (1.0 / nodes))
        w = (jnp.abs(p - nodes / 2) - nodes / 4) * step
        w2 = w * w
        poly = -2.5052108e-08
        for c in (2.7557319e-06, -1.9841270e-04, 8.3333333e-03, -1.6666667e-01):
            poly = poly * w2 + c
        return w + w * (w2 * poly)

    j = lax.broadcasted_iota(jnp.int32, (1, LANES), 1).astype(F32)
    turn = nodes // 4
    for base in range(0, count, 2 * chips):
        for at in range(base, base + chips, 16):
            wave = jnp.broadcast_to(z[at : at + 16], (16, LANES))
            phase = wave * j
            real, imag = cosine(phase), cosine(phase + turn)
            ahead = wave * LANES
            keep_part, swap_part = cosine(ahead), cosine(ahead + turn)
            for b in range(0, nodes, LANES):
                n = min(LANES, nodes - b)
                table_ref[at : at + 16, b : b + n] = real[:, :n].astype(BF16)
                table_ref[at + chips : at + chips + 16, b : b + n] = imag[:, :n].astype(BF16)
                real, imag = (
                    real * keep_part - imag * swap_part,
                    imag * keep_part + real * swap_part,
                )
    keep = pltpu.make_async_copy(table_ref, table_far, sems.at[3])
    keep.start()
    for copy in copies:
        copy.wait()
    spectra = dot(table_ref[...], x_vmem[...], ((1,), (1,))) * nodes**-0.5
    for q in range(2):
        send_ref[:, q, :] = spectra[q * group : (q + 1) * group].astype(BF16)
    keep.wait()


def basis_kernel(chips, where_ref, p_ref, v_ref, basis_ref, obs_ref, p_vmem, v_vmem, mine, sems):
    slot = where_ref[0]
    core = where_ref[2]
    first = pltpu.make_async_copy(p_ref, p_vmem, sems.at[0])
    second = pltpu.make_async_copy(v_ref.at[:, where_ref[1]], v_vmem, sems.at[1])
    first.start()
    second.start()
    degrees, _, lines = p_vmem.shape
    first.wait()
    step = 16

    def pick(start, size):
        both = p_vmem[pl.ds(start, size)].astype(F32)
        chosen = jnp.where(slot == 0, both[:, 0, :], both[:, 1, :])
        mine[pl.ds(start, size), :] = chosen.astype(BF16)

    def one(i, carry):
        pick(pl.multiple_of(i * step, step), step)
        return carry

    lax.fori_loop(0, degrees // step, one, 0)
    rest = degrees % step
    if rest:
        pick(degrees - rest, rest)
    rows = lines // (2 * chips)
    source = lax.broadcasted_iota(jnp.int32, (lines, lines), 0)
    target = lax.broadcasted_iota(jnp.int32, (lines, lines), 1)
    other = lax.div(target, lines // 2)
    their_core = core + other - 2 * core * other
    row = lax.div(lax.rem(target, lines // 2), chips)
    line = rows * (2 * lax.rem(target, chips) + their_core) + row
    order = source == line
    turned = dot(mine[...], order.astype(F32).astype(BF16), ((1,), (0,)))
    basis_ref[:degrees, :] = turned.astype(BF16)
    basis_ref[degrees:, :] = jnp.zeros((basis_ref.shape[0] - degrees, lines), BF16)
    second.wait()
    seen = v_vmem[...]
    obs_ref[...] = jnp.zeros(obs_ref.shape, F32)
    obs_ref[: seen.shape[0], :degrees] = jnp.where(slot == 0, seen[:, 0, :], seen[:, 1, :])


def swap_groups(parts, chips):
    lane = lax.broadcasted_iota(jnp.int32, parts[0].shape, 1)
    for distance in (2, 1):
        low = lax.rem(lax.div(lane, chips * distance), 2) == 0
        shift = chips * distance
        out = [None] * 4
        for j in range(4):
            if j & distance:
                continue
            a, b = parts[j], parts[j + distance]
            out[j] = jnp.where(low, a, pltpu.roll(b, shift, 1))
            out[j + distance] = jnp.where(low, pltpu.roll(a, LANES - shift, 1), b)
        parts = out
    return parts


def turn_lines(ref, q, turned, spectra, chips, ens, variables):
    local = MEMBERS // ens
    span = variables * 8
    turned[...] = ref[:, q, :].astype(F32).T
    for h in range(2):
        for m in range(local):
            parts = [turned[pl.ds(m * span + 4 * h + j, VROWS, stride=8), :] for j in range(4)]
            for k, part in enumerate(swap_groups(parts, chips)):
                e = k * local + m
                spectra[pl.ds(e * VROWS, VROWS), pl.ds(h * LANES, LANES)] = part
    return spectra[...].astype(BF16)


def own_kernel(chips, ens, variables, own_ref, basis_ref, coeffs_ref, turned, spectra):
    lines = basis_ref.shape[1]
    members = turn_lines(own_ref, 0, turned, spectra, chips, ens, variables)
    coeffs_ref[...] = dot(members, basis_ref[:, : lines // 2], ((1,), (1,)))


def crps_kernel(
    chips, ens, degrees, variables,
    z_ref, partner_ref, own_coeffs_ref, obs_ref, basis_ref, send_ref,
    turned, spectra, coeffs, grads, back,
):
    local = MEMBERS // ens
    span = variables * 8
    half = basis_ref.shape[1] // 2
    members = turn_lines(partner_ref, 1, turned, spectra, chips, ens, variables)
    coeffs[...] = own_coeffs_ref[...] + dot(members, basis_ref[:, half:], ((1,), (1,)))

    zonal = z_ref[0]
    factor = jnp.where(zonal == 0, 1.0, 2.0).astype(F32)
    tiles = VROWS // 8

    def one_block(b, totals):
        lanes = pl.ds(pl.multiple_of(b * LANES, LANES), LANES)
        degree = b * LANES + lax.broadcasted_iota(jnp.int32, (8, LANES), 1)
        active = (degree >= zonal) & (degree < degrees)
        sums = []
        for tile in range(tiles):
            c = [coeffs[pl.ds(e * VROWS + tile * 8, 8), lanes] for e in range(MEMBERS)]
            seen = obs_ref[pl.ds(tile * 8, 8), lanes]
            slope = [None] * MEMBERS
            spread = None
            inverses = None
            for e in range(MEMBERS - 1):
                for f in range(e + 1, MEMBERS):
                    gap = c[e] - c[f]
                    inverse = lax.rsqrt(gap * gap + SMOOTH * SMOOTH)
                    sign = gap * inverse
                    inverses = inverse if inverses is None else inverses + inverse
                    slope[e] = sign if slope[e] is None else slope[e] + sign
                    slope[f] = -sign if slope[f] is None else slope[f] - sign
            for e in range(1, MEMBERS):
                part = (c[e] - c[0]) * slope[e]
                spread = part if spread is None else spread + part
            pairs = MEMBERS * (MEMBERS - 1) // 2
            spread = spread + (inverses * (SMOOTH * SMOOTH) - SMOOTH * pairs)
            miss = None
            for e in range(MEMBERS):
                gap = c[e] - seen
                square = gap * gap + SMOOTH * SMOOTH
                inverse = lax.rsqrt(square)
                root = square * inverse
                miss = root if miss is None else miss + root
                grad = factor * (gap * inverse * (1 / MEMBERS) - slope[e] * (1 / MEMBERS**2))
                grad = jnp.where(active, grad, 0.0)
                grads[pl.ds(e * VROWS + tile * 8, 8), lanes] = grad.astype(BF16)
            miss = miss - SMOOTH * MEMBERS
            score = miss * (1 / MEMBERS) - spread * (1 / MEMBERS**2)
            sums.append(totals[tile] + jnp.where(active, factor * score, 0.0))
        return tuple(sums)

    blocks = coeffs.shape[1] // LANES
    zero = jnp.zeros((8, LANES), F32)
    totals = lax.fori_loop(0, blocks, one_block, (zero,) * tiles, unroll=6)

    returned = dot(grads[...], basis_ref[...], ((1,), (0,)))
    for m in range(local):
        for q in range(2):
            for h in range(2):
                at = (2 * q + h) * LANES
                parts = []
                for k in range(ens):
                    e = k * local + m
                    parts.append(returned[e * VROWS : (e + 1) * VROWS, at : at + LANES])
                for j, part in enumerate(swap_groups(parts, chips)):
                    back[q, pl.ds(m * span + 4 * h + j, VROWS, stride=8), :] = part
    base = local * span
    for tile in range(tiles):
        rest = jnp.sum(totals[tile], axis=1, keepdims=True) * (1.0 / degrees)
        for q in range(2):
            piece = rest.astype(BF16).astype(F32)
            rest = rest - piece
            back[q, pl.ds(base + tile * 8, 8), :] = jnp.broadcast_to(piece, (8, LANES))
    for q in range(2):
        back[q, base + VROWS :, :] = jnp.zeros((WIDTH - base - VROWS, LANES), F32)
        send_ref[:, q, :] = back[q].T.astype(BF16)


def score_kernel(chips, ens, variables, rows, at_ref, own_ref, turned_ref, score_ref):
    turned_ref[...] = own_ref[:, 0, :].astype(F32).T.astype(BF16)
    base = WIDTH - LANES
    mine = lax.broadcasted_iota(jnp.int32, (chips, LANES), 0) == at_ref[0]
    for k in range(ens):
        total = None
        for q in range(2):
            term = own_ref[k * chips : (k + 1) * chips, q, base:].astype(F32)
            term = jnp.sum(jnp.where(mine, term, 0.0), axis=0, keepdims=True)
            total = term if total is None else total + term
        total = pltpu.roll(total, LANES - (rows - base), 1)
        score_ref[k % 2, k // 2 : k // 2 + 1, :] = total[:, :variables]


def grid_kernel(partner_ref, own_ref, table_ref, out_ref, block, sems):
    rows, nodes = out_ref.shape
    scale = nodes**-0.5
    partner = partner_ref[:, 1, :].astype(F32).T.astype(BF16)
    turned = jnp.concatenate([own_ref[...], partner], axis=1)
    copies = []
    for a in range(0, rows, LANES):
        n = min(LANES, rows - a)
        part = dot(turned[a : a + n, :], table_ref[...], ((1,), (0,))) * scale
        block[a : a + n, :] = part.astype(BF16)
        copy = pltpu.make_async_copy(block.at[pl.ds(a, n)], out_ref.at[pl.ds(a, n)], sems.at[len(copies)])
        copy.start()
        copies.append(copy)
    for copy in copies:
        copy.wait()


def far_of(*arrays):
    return [pltpu.with_memory_space_constraint(a, pltpu.HBM) for a in arrays]


def to_chips(values):
    return lax.all_to_all(values, GROUP, 0, 0, tiled=True)


def from_partner(values):
    return lax.ppermute(values, "core", [(0, 1), (1, 0)])


def body(predicted_grid, verifying_coefficients, weighted_polynomial_values, zonal_order_values):
    local, variables, lines, nodes = predicted_grid.shape
    slots, all_lines, degrees = weighted_polynomial_values.shape
    chips = lax.axis_size("chip")
    ens = lax.axis_size("ens")
    group = chips * ens
    count = 2 * group
    rows = local * variables * lines
    padded = -(-degrees // LANES) * LANES
    whole = pl.BlockSpec(memory_space=VMEM)
    scalar = pl.BlockSpec(memory_space=pltpu.SMEM)
    far = pl.BlockSpec(memory_space=pltpu.HBM)
    chip = lax.axis_index("chip")
    core = lax.axis_index("core")
    at_ens = lax.axis_index("ens")
    slot = at_ens // 2
    sent = jax.ShapeDtypeStruct((group, 2, WIDTH), BF16)

    send, table = pl.pallas_call(
        functools.partial(fourier_kernel, chips),
        name="fourier",
        compiler_params=PARAMS,
        in_specs=[scalar, far, far],
        out_specs=[whole, far],
        out_shape=[sent, pltpu.HBM((count, nodes), BF16)],
        scratch_shapes=[
            VMEM((1, zonal_order_values.shape[0]), jnp.int32),
            VMEM((WIDTH, nodes), BF16),
            VMEM((count, nodes), BF16),
            pltpu.SemaphoreType.DMA((4,)),
        ],
    )(core.reshape(1), *far_of(zonal_order_values.reshape(1, -1), predicted_grid.reshape(rows, nodes)))
    own = to_chips(send)

    basis, observed = pl.pallas_call(
        functools.partial(basis_kernel, chips),
        name="basis",
        compiler_params=PARAMS,
        in_specs=[scalar, far, far],
        out_specs=[whole, whole],
        out_shape=[
            jax.ShapeDtypeStruct((padded, all_lines), BF16),
            jax.ShapeDtypeStruct((VROWS, padded), F32),
        ],
        scratch_shapes=[
            VMEM((degrees, slots, all_lines), BF16),
            VMEM((variables, slots, degrees), F32),
            VMEM((degrees, all_lines), BF16),
            pltpu.SemaphoreType.DMA((2,)),
        ],
        cost_estimate=pl.CostEstimate(flops=2 * degrees * all_lines**2, bytes_accessed=4_000_000, transcendentals=0),
    )(
        jnp.stack([slot, at_ens % 2, core]),
        *far_of(weighted_polynomial_values.transpose(2, 0, 1), verifying_coefficients),
    )
    own_wave = lax.dynamic_slice_in_dim(zonal_order_values, 2 * (2 * chip + core) + slot, 1)
    own, basis, observed, own_wave = lax.optimization_barrier((own, basis, observed, own_wave))
    partner = from_partner(own)

    own_coeffs = pl.pallas_call(
        functools.partial(own_kernel, chips, ens, variables),
        name="own",
        compiler_params=PARAMS,
        in_specs=[whole, whole],
        out_specs=whole,
        out_shape=jax.ShapeDtypeStruct((MEMBERS * VROWS, padded), F32),
        scratch_shapes=[VMEM((WIDTH, LANES), F32), VMEM((MEMBERS * VROWS, all_lines // 2), F32)],
        cost_estimate=pl.CostEstimate(
            flops=MEMBERS * VROWS * all_lines * degrees, bytes_accessed=2_000_000, transcendentals=0
        ),
    )(own, basis)
    send = pl.pallas_call(
        functools.partial(crps_kernel, chips, ens, degrees, variables),
        name="crps",
        compiler_params=PARAMS,
        in_specs=[scalar, whole, whole, whole, whole],
        out_specs=whole,
        out_shape=sent,
        scratch_shapes=[
            VMEM((WIDTH, LANES), F32),
            VMEM((MEMBERS * VROWS, all_lines // 2), F32),
            VMEM((MEMBERS * VROWS, padded), F32),
            VMEM((MEMBERS * VROWS, padded), BF16),
            VMEM((2, WIDTH, LANES), F32),
        ],
    )(own_wave, partner, own_coeffs, observed, basis)
    own = to_chips(send)
    partner = from_partner(own)

    turned, scores = pl.pallas_call(
        functools.partial(score_kernel, chips, ens, variables, rows),
        name="score",
        compiler_params=PARAMS,
        in_specs=[scalar, whole],
        out_specs=[whole, whole],
        out_shape=[
            jax.ShapeDtypeStruct((WIDTH, group), BF16),
            jax.ShapeDtypeStruct((2, 2, variables), F32),
        ],
        cost_estimate=pl.CostEstimate(flops=20_000_000, bytes_accessed=500_000, transcendentals=0),
    )(chip.reshape(1), own)
    sensitivity = pl.pallas_call(
        grid_kernel,
        name="grid",
        compiler_params=PARAMS,
        in_specs=[whole, whole, whole],
        out_specs=far,
        out_shape=jax.ShapeDtypeStruct((rows, nodes), BF16),
        scratch_shapes=[VMEM((rows, nodes), BF16), pltpu.SemaphoreType.DMA((5,))],
    )(partner, turned, table)
    return sensitivity.reshape(predicted_grid.shape), scores.transpose(2, 0, 1)


def solution(mesh):
    lat, ens = mesh.devices.shape
    fine = Mesh(mesh.devices.reshape(lat // 2, 2, ens), ("chip", "core", "ens"))
    block = ("chip", "core")
    placed = (P("ens", None, block, None), P(None, None, block, None), P(block, None, None), P())
    return jax.shard_map(
        body,
        mesh=fine,
        in_specs=placed,
        out_specs=(P("ens", None, block, None), P(None, None, block)),
        check_vma=False,
    )
```
